256 devices in a mesh: groups: 2 (over z), expert: 16 (over x, core), cuts: 8 (over y).
Axes of the slice: x: 8, y: 8, z: 2, core: 2. Of those that a mesh axis runs over, the one named last changes fastest.
The devices are a block of a 8x8x16 slice.
Arguments:
- tokens: bfloat16 [16384, 2048], P(('groups', 'expert')), parts along dimension 0, may hold values from -6 to 6
- route: int32 [16384, 1], P(('groups', 'expert')), parts along dimension 0, may hold values from 0 to 15; in each aligned block of 512 rows (0 to 511, 512 to 1023, ...) at most 48 rows name the same one
- gate_prob: float32 [16384], P(('groups', 'expert')), parts along dimension 0, may hold values from 0.2 to 1
- norm_gain: float32 [2048], replicated, may hold values from 0.5 to 1.5
- dense_in: bfloat16 [2048, 8192], P('expert', 'cuts'), may hold values from -0.125 to 0.125
- dense_out: bfloat16 [8192, 2048], P('cuts', 'expert'), may hold values from -0.0625 to 0.0625
- expert_in: bfloat16 [16, 2048, 8192], P('expert', None, 'cuts'), may hold values from -0.125 to 0.125
- expert_out: bfloat16 [16, 8192, 2048], P('expert', 'cuts'), may hold values from -0.0625 to 0.0625
Outputs:
- layer_out: bfloat16 [16384, 2048], P(('groups', 'expert'), 'cuts'), parts along dimension 0
The draws below stay inside these ranges and needn't reach their ends.
There are 2 independent parts, one for each index of `groups`. The reference program is written for one: setup_inputs(seed, part) draws one part's arguments, and reference() takes and returns one part's arrays. A program takes and returns all parts, laid end to end along the dimension named above; an argument that names none is the same for every part. Nothing has to cross between parts.
Inputs may be any that keep to these rules, and one draw needn't show every extreme that they name: `route`: within the rows of one device (aligned blocks of 512 rows) no expert is named by more than 48 rows; in some blocks one expert is named by exactly 48 rows.
All inputs are finite; a program needn't handle non-finite values.
Results may differ from the reference program's by a relative error of at most 0.0095.
Values may be sent and summed in bfloat16 or wider, within the bound.
A program may use at most 64 MiB of HBM per device.

```python
import math
import jax
import jax.numpy as jnp
import numpy as np
from jax import lax

D = 2048
FF = 8192
TOK_E = 512
EXPERTS = 16
CAP = 48
TOKENS = 8192
N_EXPERT = 16
N_CUTS = 8


def levels(stream_key, dims, shards, least, top_value):
    def one(dim, shards_of):
        draws = jax.random.uniform(jax.random.fold_in(jax.random.fold_in(stream_key, 6), dim), (shards_of,), jnp.float32, least / len(shards), top_value / len(shards))
        return jnp.repeat(jnp.exp(draws), dims[dim] // shards_of).reshape((-1,) + (1,) * (len(dims) - dim - 1))

    factor_of = one(*shards[0])
    for cut in shards[1:]:
        factor_of = factor_of * one(*cut)
    return factor_of


def shared_out(stream_key, own, number, rows, amount, top, limit, skew):
    sequence = jax.random.permutation(stream_key, amount)
    crowded, usual = portions_of(amount, rows * top, limit, skew, True), portions_of(amount, rows * top, limit, skew, False)
    places = jnp.arange(amount)

    def named(tallies, rotation):
        used = int((tallies > 0).sum())
        fixed = max(1, used // 4)
        shifted = fixed + (places - fixed + rotation * (used - fixed)) % max(1, amount - fixed)
        return jnp.zeros((amount,), jnp.int32).at[sequence[jnp.where(places < fixed, places, shifted)]].set(jnp.asarray(tallies, jnp.int32))

    tallies = jnp.where(number % 4 == 0, named(crowded, number // 4), named(usual, number - number // 4 - 1))
    mixed = jax.random.permutation(jax.random.fold_in(own, 3), amount)
    donor, sink = mixed[0:amount // 2 * 2:2], mixed[1:amount // 2 * 2:2]
    margin = jnp.minimum(tallies[donor] - 1, limit - tallies[sink]) // 2
    margin = jnp.where((donor == sequence[0]) | (sink == sequence[0]) | (tallies[sink] == 0), 0, jnp.maximum(margin, 0))
    shifted = jax.random.randint(jax.random.fold_in(own, 4), (amount // 2,), 0, 1 << 20) % (margin + 1)
    tallies = tallies.at[donor].add(-shifted).at[sink].add(shifted)
    items = jnp.searchsorted(jnp.cumsum(tallies), jnp.arange(rows * top), side="right").astype(jnp.int32)
    listing = items.reshape(top, rows).T
    listing = listing[jax.random.permutation(jax.random.fold_in(own, 1), rows)]
    rotation = jax.random.randint(jax.random.fold_in(own, 2), (rows, 1), 0, top)
    return jnp.take_along_axis(listing, (jnp.arange(top)[None, :] + rotation) % top, axis=1)


def portions_of(number_of, total, reach, skew, full):
    weights = [(1 << 20) // math.isqrt(rank ** skew) + 1 for rank in range(1, number_of + 1)]
    largest = reach if full else min(reach, max(-(-total // number_of), total * weights[0] // sum(weights)))
    least = 1 if total - largest >= number_of - 1 else 0
    counts, surplus = [largest] + [least] * (number_of - 1), total - largest - least * (number_of - 1)
    while surplus > 0:
        free = [i for i in range(1, number_of) if counts[i] < largest] or [i for i in range(1, number_of) if counts[i] < reach]
        mass, left = sum([weights[i] for i in free]), surplus
        for i in free:
            more = min(reach - counts[i], max(1, left * weights[i] // mass), surplus)
            counts[i] = counts[i] + more
            surplus = surplus - more
    return np.array(counts)


def normal_values(rng, dims, deviation, bound, shards=(), kind=jnp.bfloat16):
    drawn = deviation * jax.random.normal(rng, dims, jnp.float32)
    if shards:
        drawn = drawn * levels(rng, dims, shards, -0.22, 0.18)
    return jnp.clip(drawn, -bound, bound).astype(kind)


def setup_inputs(seed: int = 0, part: int = 0) -> dict:
    arg_keys = jax.random.split(jax.random.key(seed), 9)
    part_keys = jax.random.split(jax.random.fold_in(arg_keys[8], part), 9)
    tokens = normal_values(part_keys[0], (TOKENS, D), 1.0, 6.0, ((0, 16),))
    route_keys = jax.random.split(jax.random.fold_in(part_keys[1], 1), TOKENS // TOK_E)
    route_turns = jax.random.permutation(jax.random.fold_in(part_keys[1], 3), TOKENS // TOK_E)
    route = jax.vmap(lambda own, number: shared_out(jax.random.fold_in(part_keys[1], 2), own, number, TOK_E, EXPERTS, 1, CAP, 2))(route_keys, route_turns).reshape((TOKENS, 1))
    gate_prob = jnp.clip(jnp.exp(math.log(1.0) - 1.609438 * jax.random.uniform(part_keys[2], (TOKENS,), jnp.float32) ** levels(part_keys[2], (TOKENS,), ((0, 16),), -0.2, 0.2)), 0.2, 1.0)
    norm_gain = jnp.clip(1.0 + 0.1 * jax.random.normal(arg_keys[3], (D,), jnp.float32), 0.5, 1.5)
    dense_in = normal_values(arg_keys[4], (D, FF), D ** -0.5, 0.125, ((0, 16), (1, 8)))
    dense_out = normal_values(arg_keys[5], (FF, D), FF ** -0.5, 0.0625, ((0, 8), (1, 16)))
    expert_in = normal_values(arg_keys[6], (EXPERTS, D, FF), D ** -0.5, 0.125, ((0, 16), (2, 8)))
    expert_out = normal_values(arg_keys[7], (EXPERTS, FF, D), FF ** -0.5, 0.0625, ((0, 16), (1, 8)))
    return {"tokens": tokens, "route": route, "gate_prob": gate_prob, "norm_gain": norm_gain, "dense_in": dense_in, "dense_out": dense_out, "expert_in": expert_in, "expert_out": expert_out}


def normalize(tokens, norm_gain):
    widened = tokens.astype(jnp.float32)
    meansq = lax.optimization_barrier(jnp.mean(widened * widened, axis=-1, keepdims=True))
    return (widened * lax.rsqrt(meansq + 1e-06) * norm_gain).astype(jnp.bfloat16)

def sliced_product(act, weight):
    rows = act.shape[0]
    width = FF // N_CUTS
    act_parts = act.reshape(rows, N_CUTS, width).transpose(1, 0, 2)
    weight_parts = weight.reshape(N_CUTS, width, D)

    def add_slice(total, operands):
        act_part, weight_part = operands
        partial_out = jnp.dot(act_part, weight_part, preferred_element_type=jnp.float32)
        rounded = lax.optimization_barrier(partial_out.astype(jnp.bfloat16)).astype(jnp.float32)
        return (total + rounded, None)
    total, unused = lax.scan(add_slice, jnp.zeros((rows, D), jnp.float32), (act_parts, weight_parts))
    return total

def run_expert(operands):
    gathered, weight_in, weight_out = operands
    inner = jax.nn.gelu(jnp.dot(gathered, weight_in, preferred_element_type=jnp.float32)).astype(jnp.bfloat16)
    return sliced_product(inner, weight_out).astype(jnp.bfloat16)

def reference(tokens, route, gate_prob, norm_gain, dense_in, dense_out, expert_in, expert_out):
    normed = normalize(tokens, norm_gain)
    dense_act = jax.nn.gelu(jnp.dot(normed, dense_in, preferred_element_type=jnp.float32)).astype(jnp.bfloat16)
    dense = sliced_product(dense_act, dense_out)
    picked = route[:, 0].reshape(N_EXPERT, TOK_E)
    labels = jnp.arange(EXPERTS, dtype=jnp.int32)
    one_hot = (picked[:, :, None] == labels[None, None, :]).astype(jnp.int32)
    before = jnp.cumsum(one_hot, axis=1) - one_hot
    position = lax.optimization_barrier(jnp.sum(before * one_hot, axis=-1))
    block_ids = jnp.arange(N_EXPERT, dtype=jnp.int32)[:, None]
    target = (picked * (N_EXPERT * CAP) + block_ids * CAP + position).reshape(-1).astype(jnp.int32)
    buffer = jnp.zeros((EXPERTS * N_EXPERT * CAP, D), jnp.bfloat16).at[target].set(normed)
    buffer = buffer.reshape(EXPERTS, N_EXPERT * CAP, D)
    results = lax.map(run_expert, (buffer, expert_in, expert_out)).reshape(-1, D)
    expert_res = results[target].astype(jnp.float32)
    layer_out = tokens.astype(jnp.float32) + dense + gate_prob[:, None] * expert_res
    return layer_out.astype(jnp.bfloat16)
```

```python
import functools

import jax
import jax.numpy as jnp
from jax import lax
from jax.experimental import pallas as pl
from jax.experimental.pallas import tpu as pltpu
from jax.sharding import PartitionSpec as P

MESH = pl.DeviceIdType.MESH
F32 = jnp.float32
BF16 = jnp.bfloat16
CHUNKS = 4


def layer_kernel(
    dims,
    tokens_hbm,
    route_ref,
    gate_ref,
    gain_ref,
    dense_in_hbm,
    dense_out_hbm,
    expert_in_hbm,
    expert_out_hbm,
    out_ref,
    tok,
    norm,
    pick,
    outgoing,
    arrived,
    w_in,
    w_out,
    d_in,
    d_out,
    inner,
    part,
    part_in,
    result,
    returned,
    dense_act,
    dense_part,
    dense_part_in,
    load_sem,
    disp_send,
    disp_recv,
    gath_send,
    gath_recv,
    ring_send,
    ring_recv,
    sib_send,
    sib_recv,
    red_send,
    red_recv,
    ret_send,
    ret_recv,
    dred_send,
    dred_recv,
):
    n_exp, n_cut, cap, rows, width, share, hidden = dims
    n_chip = n_exp // 2
    half_x, half_y = n_chip // 2, n_cut // 2
    per_chunk = n_exp // CHUNKS
    chunk_rows = per_chunk * cap
    drows = rows // CHUNKS
    offsets = [0] + [(p + 1) // 2 if p % 2 else -(p // 2) for p in range(1, n_chip)]

    e = lax.axis_index("expert")
    c = lax.axis_index("cuts")
    x = e // 2
    core = e - 2 * x
    sibling = 2 * x + 1 - core

    def chip(offset):
        return lax.rem(x + offset + n_chip, n_chip)

    def cut(offset):
        return lax.rem(c + offset + n_cut, n_cut)

    started = []

    def send(src, dst, send_sem, recv_sem, device):
        copy = pltpu.make_async_remote_copy(
            src_ref=src,
            dst_ref=dst,
            send_sem=send_sem,
            recv_sem=recv_sem,
            device_id=device,
            device_id_type=MESH,
        )
        copy.start()
        started.append(copy)

    def arrive(dst, recv_sem, send_sem):
        pltpu.make_async_remote_copy(
            src_ref=dst,
            dst_ref=dst,
            send_sem=send_sem,
            recv_sem=recv_sem,
            device_id={"expert": sibling},
            device_id_type=MESH,
        ).wait_recv()

    loads = []
    for number, (src, dst) in enumerate(
        (
            (tokens_hbm, tok),
            (dense_in_hbm, d_in.at[x, core]),
            (dense_out_hbm, d_out.at[x, core]),
            (expert_in_hbm, w_in),
            (expert_out_hbm, w_out),
        )
    ):
        copy = pltpu.make_async_copy(src, dst, load_sem.at[number])
        copy.start()
        loads.append(copy)

    barrier = pltpu.get_barrier_semaphore()
    for step in range(1, n_exp):
        pl.semaphore_signal(
            barrier, inc=1, device_id={"expert": lax.rem(e + step, n_exp)}, device_id_type=MESH
        )
    for step in (1, -1):
        pl.semaphore_signal(barrier, inc=1, device_id={"cuts": cut(step)}, device_id_type=MESH)

    route = route_ref[...]
    hot = lax.broadcasted_iota(jnp.int32, (n_exp, rows), 0) == route
    hot = jnp.where(hot, 1.0, 0.0).astype(F32)
    earlier = lax.broadcasted_iota(jnp.int32, (rows, rows), 0) < lax.broadcasted_iota(
        jnp.int32, (rows, rows), 1
    )
    earlier = jnp.where(earlier, 1.0, 0.0).astype(BF16)
    before = jnp.dot(hot.astype(BF16), earlier, preferred_element_type=F32)
    position = jnp.sum(before * hot, axis=0, keepdims=True)
    target = route * cap + position.astype(jnp.int32)
    slots = lax.broadcasted_iota(jnp.int32, (n_exp * cap, rows), 0)
    pick[...] = jnp.where(slots == target, 1.0, 0.0).astype(BF16)

    loads[0].wait()
    block = rows // 8

    @pl.loop(0, 8)
    def _(i):
        here = pl.ds(pl.multiple_of(i * block, block), block)
        wide = tok[here, :].astype(F32)
        meansq = jnp.mean(wide * wide, axis=-1, keepdims=True)
        norm[here, :] = (wide * lax.rsqrt(meansq + 1e-06) * gain_ref[...]).astype(BF16)

    own_columns = pl.ds(pl.multiple_of(c * share, share), share)
    outgoing[...] = (
        jnp.dot(pick[...], norm[:, own_columns], preferred_element_type=F32)
        .astype(BF16)
        .reshape(n_exp, cap, share)
    )
    arrived[c, core] = outgoing[e]
    pl.semaphore_wait(barrier, n_exp + 1)

    for p in range(n_chip):
        if p == 0:
            send(
                outgoing.at[sibling],
                arrived.at[c, core],
                disp_send.at[0],
                disp_recv.at[core],
                {"expert": sibling},
            )
            continue
        for k in range(2):
            to = 2 * chip(-offsets[p]) + k
            send(
                outgoing.at[to],
                arrived.at[c, 2 * p + core],
                disp_send.at[2 * p + k],
                disp_recv.at[2 * p + core],
                {"expert": to},
            )

    weights = (d_in, d_out)

    def ring_device(way):
        return {"expert": 2 * chip(1 if way == 0 else -1) + core}

    def ring_own(w):
        own = weights[w].at[x, core]
        for way in range(2):
            send(own, own, ring_send.at[way, w, 0], ring_recv.at[way, w, 0], ring_device(way))
        send(own, own, sib_send.at[w, 0], sib_recv.at[w, 0], {"expert": sibling})

    def ring_event(w, hop):
        for way in range(2):
            if hop == half_x and w != way:
                continue
            origin = chip(-hop if way == 0 else hop)
            piece = weights[w].at[origin, core]
            arrive(piece, ring_recv.at[way, w, hop - 1], ring_send.at[way, w, 0])
            if hop < half_x - 1 or (hop == half_x - 1 and w == way):
                send(
                    piece,
                    piece,
                    ring_send.at[way, w, hop],
                    ring_recv.at[way, w, hop],
                    ring_device(way),
                )
            place = hop if way == 0 else n_chip - hop
            send(piece, piece, sib_send.at[w, place], sib_recv.at[w, place], {"expert": sibling})

    ring_events = [(w, hop) for hop in range(1, half_x + 1) for w in range(2)]

    def ring_next():
        if ring_events:
            ring_event(*ring_events.pop(0))

    loads[1].wait()
    loads[2].wait()
    ring_own(0)
    ring_own(1)

    def cut_device(way):
        return {"cuts": cut(1 if way == 0 else -1)}

    def chunk_slots(r):
        return pl.ds(r * per_chunk, per_chunk)

    def gather_event(hop, r):
        if hop == 0:
            for slot in range(r * per_chunk, (r + 1) * per_chunk):
                if slot == 0:
                    other = 1 - core
                    arrive(arrived.at[c, other], disp_recv.at[other], disp_send.at[0])
                elif slot > 1:
                    arrive(arrived.at[c, slot], disp_recv.at[slot], disp_send.at[0])
        for way in range(2):
            if hop == half_y and r % 2 != way:
                continue
            origin = cut(-hop if way == 0 else hop)
            piece = arrived.at[origin, chunk_slots(r)]
            if hop > 0:
                arrive(piece, gath_recv.at[way, hop - 1, r], gath_send.at[way, 0, 0])
            if hop < half_y - 1 or (hop == half_y - 1 and r % 2 == way):
                send(
                    piece,
                    piece,
                    gath_send.at[way, hop, r],
                    gath_recv.at[way, hop, r],
                    cut_device(way),
                )

    for hop in range(half_y):
        for r in range(CHUNKS):
            gather_event(hop, r)
            if (hop, r) in ((2, 0), (2, 3), (3, 2)):
                ring_next()

    def expert_chunk(r):
        here = chunk_slots(r)
        flat = jnp.concatenate(
            [arrived[k, here].reshape(chunk_rows, share) for k in range(n_cut)], axis=1
        )
        for n in range(2):
            columns = pl.ds(n * (hidden // 2), hidden // 2)
            inner[:, columns] = jax.nn.gelu(
                jnp.dot(flat, w_in[:, columns], preferred_element_type=F32)
            ).astype(BF16)
        for k in range(n_cut):
            part[k, here] = (
                jnp.dot(
                    inner[...], w_out[:, pl.ds(k * share, share)], preferred_element_type=F32
                )
                .astype(BF16)
                .reshape(per_chunk, cap, share)
            )

    def reduce_event(own, landed, send_sem, recv_sem, here, step, r):
        for way in range(2):
            if step == half_y and r % 2 != way:
                continue
            home = cut(step if way == 0 else -step)
            if step == half_y or (step == half_y - 1 and r % 2 != way):
                piece = own.at[home, here]
            else:
                piece = landed.at[way, step, here]
                arrive(piece, recv_sem.at[way, step, r], send_sem.at[way, 0, r])
                landed[way, step, here] = (
                    landed[way, step, here].astype(F32) + own[home, here].astype(F32)
                ).astype(BF16)
            send(
                piece,
                landed.at[way, step - 1, here],
                send_sem.at[way, step - 1, r],
                recv_sem.at[way, step - 1, r],
                cut_device(way),
            )

    def reduce_last(own, landed, send_sem, recv_sem, here, r):
        total = own[c, here].astype(F32)
        for way in range(2):
            arrive(landed.at[way, 0, here], recv_sem.at[way, 0, r], send_sem.at[way, 0, r])
            total = total + landed[way, 0, here].astype(F32)
        return total

    def expert_reduce(step, r):
        reduce_event(part, part_in, red_send, red_recv, chunk_slots(r), step, r)

    loads[3].wait()
    loads[4].wait()
    for r in range(CHUNKS):
        gather_event(half_y, r)
        expert_chunk(r)
        expert_reduce(half_y, r)
        if r == 1:
            ring_next()
    for r in range(CHUNKS):
        expert_reduce(half_y - 1, r)
        if r in (0, 3):
            ring_next()
    for r in range(CHUNKS):
        expert_reduce(half_y - 2, r)
    while ring_events:
        ring_next()

    def dense_first(n):
        size = hidden // 4
        columns = pl.ds(n * size, size)
        dense_act[:, columns] = jax.nn.gelu(
            jnp.dot(
                norm[...],
                d_in[:, :, :, columns].reshape(width, size),
                preferred_element_type=F32,
            )
        ).astype(BF16)

    def dense_second(k):
        dense_part[k] = jnp.dot(
            dense_act[...],
            jnp.concatenate([d_out[k, 0], d_out[k, 1]], axis=1),
            preferred_element_type=F32,
        ).astype(BF16)

    for w in range(2):
        for place in range(n_chip):
            arrive(
                weights[w].at[chip(-place), 1 - core],
                sib_recv.at[w, place],
                sib_send.at[w, place],
            )
    steps = list(range(half_y - 3, 0, -1))
    for step in steps:
        for r in range(CHUNKS):
            expert_reduce(step, r)
            dense_first(r)

    def go_home(r):
        here = chunk_slots(r)
        result[here] = reduce_last(part, part_in, red_send, red_recv, here, r).astype(BF16)
        for slot in range(r * per_chunk, (r + 1) * per_chunk):
            if slot == 0:
                returned[e] = result[core]
                send(
                    result.at[1 - core],
                    returned.at[e],
                    ret_send.at[0],
                    ret_recv.at[e],
                    {"expert": sibling},
                )
            elif slot > 1:
                to = 2 * chip(offsets[slot // 2]) + slot % 2
                send(
                    result.at[slot], returned.at[e], ret_send.at[slot], ret_recv.at[e], {"expert": to}
                )

    def dense_slice(r):
        return pl.ds(r * drows, drows)

    def dense_reduce(step, r):
        reduce_event(dense_part, dense_part_in, dred_send, dred_recv, dense_slice(r), step, r)

    for k in range(n_cut):
        dense_second(k)
    for r in range(CHUNKS):
        dense_reduce(half_y, r)
    for r in range(CHUNKS):
        go_home(r)
    for step in range(half_y - 1, 0, -1):
        for r in range(CHUNKS):
            dense_reduce(step, r)

    for step in range(1, n_exp):
        sender = lax.rem(e + step, n_exp)
        arrive(returned.at[sender], ret_recv.at[sender], ret_send.at[0])
    expert_res = lax.dot_general(
        pick[...],
        returned[...].reshape(n_exp * cap, share),
        (((0,), (0,)), ((), ())),
        preferred_element_type=F32,
    )
    gate = jnp.transpose(jnp.broadcast_to(gate_ref[...], (128, rows)))[:, 0:1]
    dense_part_sum = tok[:, own_columns].astype(F32) + gate * expert_res
    for r in range(CHUNKS):
        here = dense_slice(r)
        total = reduce_last(dense_part, dense_part_in, dred_send, dred_recv, here, r)
        out_ref[here, :] = (
            dense_part_sum[r * drows : (r + 1) * drows] + total
        ).astype(BF16)

    for copy in started:
        copy.wait_send()


def local(tokens, route, gate_prob, norm_gain, dense_in, dense_out, expert_in, expert_out):
    n_exp = lax.axis_size("expert")
    n_cut = lax.axis_size("cuts")
    rows, width = tokens.shape
    share = width // n_cut
    hidden = expert_in.shape[2]
    cap = max(2, 3 * rows // (2 * n_exp))
    n_chip = n_exp // 2
    depth = dense_in.shape[0]
    half_y = n_cut // 2
    dims = (n_exp, n_cut, cap, rows, width, share, hidden)
    vmem = pl.BlockSpec(memory_space=pltpu.VMEM)
    hbm = pl.BlockSpec(memory_space=pl.ANY)
    dma = pltpu.SemaphoreType.DMA
    return pl.pallas_call(
        functools.partial(layer_kernel, dims),
        out_shape=jax.ShapeDtypeStruct((rows, share), BF16),
        in_specs=[hbm, vmem, vmem, vmem, hbm, hbm, hbm, hbm],
        out_specs=vmem,
        scratch_shapes=[
            pltpu.VMEM((rows, width), BF16),
            pltpu.VMEM((rows, width), BF16),
            pltpu.VMEM((n_exp * cap, rows), BF16),
            pltpu.VMEM((n_exp, cap, share), BF16),
            pltpu.VMEM((n_cut, n_exp, cap, share), BF16),
            pltpu.VMEM((width, hidden), BF16),
            pltpu.VMEM((hidden, width), BF16),
            pltpu.VMEM((n_chip, 2, depth, hidden), BF16),
            pltpu.VMEM((n_chip, 2, hidden, depth), BF16),
            pltpu.VMEM((n_exp // CHUNKS * cap, hidden), BF16),
            pltpu.VMEM((n_cut, n_exp, cap, share), BF16),
            pltpu.VMEM((2, half_y, n_exp, cap, share), BF16),
            pltpu.VMEM((n_exp, cap, share), BF16),
            pltpu.VMEM((n_exp, cap, share), BF16),
            pltpu.VMEM((rows, hidden), BF16),
            pltpu.VMEM((n_cut, rows, share), BF16),
            pltpu.VMEM((2, half_y, rows, share), BF16),
            dma((5,)),
            dma((n_exp,)),
            dma((n_exp,)),
            dma((2, half_y, CHUNKS)),
            dma((2, half_y, CHUNKS)),
            dma((2, 2, n_chip // 2)),
            dma((2, 2, n_chip // 2)),
            dma((2, n_chip)),
            dma((2, n_chip)),
            dma((2, half_y, CHUNKS)),
            dma((2, half_y, CHUNKS)),
            dma((n_exp,)),
            dma((n_exp,)),
            dma((2, half_y, CHUNKS)),
            dma((2, half_y, CHUNKS)),
        ],
        compiler_params=pltpu.CompilerParams(
            collective_id=0, has_side_effects=True, vmem_limit_bytes=60 * 1024 * 1024
        ),
        name="moe_layer",
    )(
        tokens,
        route.reshape(1, rows),
        gate_prob.reshape(1, rows),
        norm_gain.reshape(1, width),
        dense_in,
        dense_out,
        expert_in.reshape(width, hidden),
        expert_out.reshape(hidden, width),
    )


def solution(mesh):
    return jax.shard_map(
        local,
        mesh=mesh,
        in_specs=(
            P(("groups", "expert"), None),
            P(("groups", "expert"), None),
            P(("groups", "expert")),
            P(),
            P("expert", "cuts"),
            P("cuts", "expert"),
            P("expert", None, "cuts"),
            P("expert", "cuts", None),
        ),
        out_specs=P(("groups", "expert"), "cuts"),
        check_vma=False,
    )
```

```python
import functools

import jax
import jax.numpy as jnp
from jax import lax
from jax.experimental import pallas as pl
from jax.experimental.pallas import tpu as pltpu
from jax.sharding import PartitionSpec as P

MESH = pl.DeviceIdType.MESH
F32 = jnp.float32
BF16 = jnp.bfloat16
CHUNKS = 4


def layer_kernel(
    dims,
    tokens_hbm,
    route_ref,
    gate_ref,
    gain_ref,
    dense_in_hbm,
    dense_out_hbm,
    expert_in_hbm,
    expert_out_hbm,
    out_ref,
    tok,
    norm,
    pick,
    pick_home,
    gate_wide,
    outgoing,
    outgoing_near,
    arrived,
    w_in,
    w_out,
    d_in,
    d_out,
    inner,
    part,
    part_near,
    part_in,
    near,
    result,
    returned,
    dense_act,
    dense_part,
    dense_part_in,
    base,
    load_sem,
    near_send,
    near_recv,
    disp_send,
    disp_recv,
    gath_send,
    gath_recv,
    ring_send,
    ring_recv,
    sib_send,
    sib_recv,
    red_send,
    red_recv,
    ret_send,
    ret_recv,
    dred_send,
    dred_recv,
):
    n_exp, n_cut, cap, rows, width, share, hidden = dims
    n_chip = n_exp // 2
    half_x, half_y = n_chip // 2, n_cut // 2
    offsets = [0] + [(p + 1) // 2 if p % 2 else -(p // 2) for p in range(1, n_chip)]
    far = n_exp - 2
    size = -(-far // CHUNKS)
    size += size % 2
    chunks = [(first, min(size, n_exp - first)) for first in range(2, n_exp, size)]
    dsize = rows // CHUNKS
    dense_chunks = [(first, dsize) for first in range(0, rows, dsize)]

    e = lax.axis_index("expert")
    c = lax.axis_index("cuts")
    x = e // 2
    core = e - 2 * x
    other = 1 - core
    sibling = {"expert": 2 * x + other}

    def chip(offset):
        return lax.rem(x + offset + n_chip, n_chip)

    def cut(offset):
        return lax.rem(c + offset + n_cut, n_cut)

    def ring_device(way):
        return {"expert": 2 * chip(1 if way == 0 else -1) + core}

    def cut_device(way):
        return {"cuts": cut(1 if way == 0 else -1)}

    def remote(src, dst, send_sem, recv_sem, device):
        return pltpu.make_async_remote_copy(
            src_ref=src,
            dst_ref=dst,
            send_sem=send_sem,
            recv_sem=recv_sem,
            device_id=device,
            device_id_type=MESH,
        )

    def send(src, dst, send_sem, recv_sem, device):
        remote(src, dst, send_sem, recv_sem, device).start()

    def arrive(dst, recv_sem, send_sem):
        remote(dst, dst, send_sem, recv_sem, sibling).wait_recv()

    def sent(src, send_sem, recv_sem):
        remote(src, src, send_sem, recv_sem, sibling).wait_send()

    def halves(chunk):
        first, count = chunk
        return (
            pl.ds(first, count // 2),
            pl.ds(first + count // 2, count // 2),
        )

    loads = []
    for number, (src, dst) in enumerate(
        (
            (tokens_hbm, tok),
            (expert_in_hbm, w_in),
            (expert_out_hbm, w_out),
            (dense_in_hbm, d_in.at[x, core]),
            (dense_out_hbm, d_out.at[x, core]),
        )
    ):
        copy = pltpu.make_async_copy(src, dst, load_sem.at[number])
        copy.start()
        loads.append(copy)

    barrier = pltpu.get_barrier_semaphore()
    for step in range(1, n_exp):
        pl.semaphore_signal(
            barrier, inc=1, device_id={"expert": lax.rem(e + step, n_exp)}, device_id_type=MESH
        )
    for way in range(2):
        pl.semaphore_signal(barrier, inc=1, device_id=cut_device(way), device_id_type=MESH)

    route = route_ref[...]
    hot = lax.broadcasted_iota(jnp.int32, (n_exp, rows), 0) == route
    hot = jnp.where(hot, 1.0, 0.0).astype(F32)
    earlier = lax.broadcasted_iota(jnp.int32, (rows, rows), 0) < lax.broadcasted_iota(
        jnp.int32, (rows, rows), 1
    )
    earlier = jnp.where(earlier, 1.0, 0.0).astype(BF16)
    before = jnp.dot(hot.astype(BF16), earlier, preferred_element_type=F32)
    position = jnp.sum(before * hot, axis=0, keepdims=True)
    target = route * cap + position.astype(jnp.int32)
    slots = lax.broadcasted_iota(jnp.int32, (n_exp * cap, rows), 0)
    pick[...] = jnp.where(slots == target, 1.0, 0.0).astype(BF16)

    loads[0].wait()
    block = rows // 8

    @pl.loop(0, 8)
    def _(i):
        here = pl.ds(pl.multiple_of(i * block, block), block)
        wide = tok[here, :].astype(F32)
        meansq = jnp.mean(wide * wide, axis=-1, keepdims=True)
        norm[here, :] = (wide * lax.rsqrt(meansq + 1e-06) * gain_ref[...]).astype(BF16)

    own_columns = pl.ds(pl.multiple_of(c * share, share), share)
    outgoing[...] = (
        jnp.dot(pick[...], norm[:, own_columns], preferred_element_type=F32)
        .astype(BF16)
        .reshape(n_exp, cap, share)
    )
    pl.semaphore_wait(barrier, n_exp + 1)

    def chunk_of(slot):
        return (slot - 2) // size

    for p in range(1, n_chip):
        for k in range(2):
            to = 2 * chip(-offsets[p]) + k
            send(
                outgoing.at[to],
                arrived.at[c, 2 * p + core],
                disp_send,
                disp_recv.at[chunk_of(2 * p)],
                {"expert": to},
            )

    near_rows = pick[pl.ds(pl.multiple_of(2 * x * cap, 2 * cap), 2 * cap), :]
    for k in range(n_cut):
        outgoing_near[k] = (
            jnp.dot(near_rows, norm[:, pl.ds(k * share, share)], preferred_element_type=F32)
            .astype(BF16)
            .reshape(2, cap, share)
        )
    send(
        outgoing_near.at[:, other], arrived.at[:, core], near_send.at[0], near_recv.at[0], sibling
    )
    for k in range(n_cut):
        arrived[k, core] = outgoing_near[k, core]

    weights = (d_in, d_out)

    def ring_own(w):
        loads[3 + w].wait()
        own = weights[w].at[x, core]
        for way in range(2):
            send(own, own, ring_send.at[w], ring_recv.at[way, w, 0], ring_device(way))
        send(own, own, sib_send.at[w], sib_recv.at[w], sibling)

    def ring_event(w, hop):
        for way in range(2):
            if hop == half_x and w != way:
                continue
            origin = chip(-hop if way == 0 else hop)
            piece = weights[w].at[origin, core]
            arrive(piece, ring_recv.at[way, w, hop - 1], ring_send.at[w])
            if hop < half_x - 1 or (hop == half_x - 1 and w == way):
                send(piece, piece, ring_send.at[w], ring_recv.at[way, w, hop], ring_device(way))
            send(piece, piece, sib_send.at[w], sib_recv.at[w], sibling)

    ring_events = [(w, hop) for hop in range(1, half_x + 1) for w in range(2)]

    def ring_next():
        ring_event(*ring_events.pop(0))

    def gather_event(hop, r):
        first, count = chunks[r]
        whole = pl.ds(first, count)
        if hop == 0:
            arrive(arrived.at[c, whole], disp_recv.at[r], disp_send)
        for way in range(2):
            here = halves(chunks[r])[way] if hop == half_y else whole
            onward = halves(chunks[r])[way] if hop == half_y - 1 else here
            origin = cut(-hop if way == 0 else hop)
            if hop > 0:
                arrive(arrived.at[origin, here], gath_recv.at[way, hop - 1, r], gath_send)
            if hop < half_y:
                piece = arrived.at[origin, onward]
                send(piece, piece, gath_send, gath_recv.at[way, hop, r], cut_device(way))

    def expert_rows(first, count, keep):
        flat = jnp.concatenate(
            [
                arrived[k, pl.ds(first, count)].reshape(count * cap, share)
                for k in range(n_cut)
            ],
            axis=1,
        )
        for n in range(2):
            columns = pl.ds(n * (hidden // 2), hidden // 2)
            inner[pl.ds(0, count * cap), columns] = jax.nn.gelu(
                jnp.dot(flat, w_in[:, columns], preferred_element_type=F32)
            ).astype(BF16)
        for k in range(0, n_cut, 2):
            both = jnp.dot(
                inner[pl.ds(0, count * cap), :],
                w_out[:, pl.ds(k * share, 2 * share)],
                preferred_element_type=F32,
            ).astype(BF16)
            for j in range(2):
                keep(k + j, both[:, j * share : (j + 1) * share].reshape(count, cap, share))

    def expert_near():
        def keep(k, values):
            part_near[k] = values

        arrive(arrived.at[:, other], near_recv.at[0], near_send.at[0])
        expert_rows(0, 2, keep)
        send(
            part_near.at[:, other], near.at[:, core], near_send.at[1], near_recv.at[1], sibling
        )
        for k in range(n_cut):
            near[k, core] = part_near[k, core]

    def expert_chunk(r):
        first, count = chunks[r]

        def keep(k, values):
            part[k, pl.ds(first, count)] = values

        expert_rows(first, count, keep)

    def reduce_event(own, landed, send_sem, recv_sem, chunk, step, r):
        whole = pl.ds(*chunk)
        for way in range(2):
            half, rest = halves(chunk)[way], halves(chunk)[1 - way]
            home = cut(step if way == 0 else -step)
            to = step - 1
            if step == half_y:
                send(
                    own.at[home, half],
                    landed.at[way, to, half],
                    send_sem,
                    recv_sem.at[way, to, r],
                    cut_device(way),
                )
                continue
            here = half if step == half_y - 1 else whole
            arrive(landed.at[way, step, here], recv_sem.at[way, step, r], send_sem)
            landed[way, step, here] = (
                landed[way, step, here].astype(F32) + own[home, here].astype(F32)
            ).astype(BF16)
            if step == half_y - 1:
                landed[way, step, rest] = own[home, rest]
            send(
                landed.at[way, step, whole],
                landed.at[way, to, whole],
                send_sem,
                recv_sem.at[way, to, r],
                cut_device(way),
            )

    def reduce_last(own, landed, send_sem, recv_sem, chunk, r):
        whole = pl.ds(*chunk)
        total = own[c, whole].astype(F32)
        for way in range(2):
            arrive(landed.at[way, 0, whole], recv_sem.at[way, 0, r], send_sem)
            total = total + landed[way, 0, whole].astype(F32)
        return total

    def expert_reduce(step, r):
        reduce_event(part, part_in, red_send, red_recv, chunks[r], step, r)

    def go_home(r):
        first, count = chunks[r]
        result[pl.ds(first, count)] = reduce_last(
            part, part_in, red_send, red_recv, chunks[r], r
        ).astype(BF16)
        for slot in range(first, first + count):
            to = 2 * chip(offsets[slot // 2]) + slot % 2
            send(result.at[slot], returned.at[e], ret_send, ret_recv, {"expert": to})

    def dense_first(n):
        columns = pl.ds(n * (hidden // 2), hidden // 2)
        dense_act[:, columns] = jax.nn.gelu(
            jnp.dot(
                norm[...],
                d_in[:, :, :, columns].reshape(width, hidden // 2),
                preferred_element_type=F32,
            )
        ).astype(BF16)

    def dense_second(k):
        both = jnp.dot(
            dense_act[...],
            jnp.concatenate([d_out[k, 0], d_out[k, 1], d_out[k + 1, 0], d_out[k + 1, 1]], axis=1),
            preferred_element_type=F32,
        )
        rows_near = jnp.concatenate(
            [near[k].reshape(2 * cap, share), near[k + 1].reshape(2 * cap, share)], axis=1
        )
        both = both + gate_wide[:, 0:1] * jnp.dot(
            near_home, rows_near, preferred_element_type=F32
        )
        both = both.astype(BF16)
        dense_part[k] = both[:, :share]
        dense_part[k + 1] = both[:, share:]

    def dense_reduce(step, r):
        reduce_event(
            dense_part, dense_part_in, dred_send, dred_recv, dense_chunks[r], step, r
        )

    def home_tables():
        gate_wide[...] = jnp.transpose(jnp.broadcast_to(gate_ref[...], (128, rows)))
        wide = jnp.transpose(jnp.broadcast_to(target.astype(F32), (128, rows)))[:, 0:1]
        slot_of = lax.broadcasted_iota(jnp.int32, (rows, n_exp * cap), 1).astype(F32)
        pick_home[...] = jnp.where(slot_of == wide, 1.0, 0.0).astype(BF16)
        slot_of = lax.broadcasted_iota(jnp.int32, (rows, 2 * cap), 1) + 2 * x * cap
        return jnp.where(slot_of.astype(F32) == wide, 1.0, 0.0).astype(BF16)

    loads[1].wait()
    loads[2].wait()
    returned[pl.ds(2 * x, 2)] = jnp.zeros((2, cap, share), BF16)
    near_home = home_tables()
    expert_near()
    last = len(chunks) - 1
    gather_event(0, 0)
    gather_event(0, 1)
    ring_own(0)
    gather_event(0, 2)
    gather_event(0, 3)
    ring_own(1)
    for hop in range(1, half_y):
        for r in range(len(chunks)):
            gather_event(hop, r)
            if (hop, r) in ((1, 2), (2, 1), (2, 3)):
                ring_next()
    for r in range(len(chunks)):
        gather_event(half_y, r)
        expert_chunk(r)
        expert_reduce(half_y, r)
        if r in (0, 2):
            ring_next()
    for step in range(half_y - 1, 0, -1):
        for r in range(len(chunks)):
            expert_reduce(step, r)
            if (step, r) in ((3, 1), (3, 3), (2, 0)):
                ring_next()
            if (step, r) == (2, 1):
                arrive(d_in.at[:, other], sib_recv.at[0], sib_send.at[0])
                dense_first(0)
            if (step, r) == (2, 2):
                dense_first(1)
            if (step, r) == (2, 3):
                arrive(d_out.at[:, other], sib_recv.at[1], sib_send.at[1])
                arrive(near.at[:, other], near_recv.at[1], near_send.at[1])
            if step == 1:
                dense_second(2 * r)
    for r in range(CHUNKS):
        dense_reduce(half_y, r)
    for r in range(len(chunks)):
        go_home(r)
    for step in range(half_y - 1, 0, -1):
        for r in range(CHUNKS):
            dense_reduce(step, r)
            if (step, r) == (1, 0):
                arrive(returned.at[pl.ds(0, far)], ret_recv, ret_send)
                expert_res = jnp.dot(
                    pick_home[...],
                    returned[...].reshape(n_exp * cap, share),
                    preferred_element_type=F32,
                )
                base[...] = tok[:, own_columns].astype(F32) + gate_wide[:, 0:1] * expert_res
    for r in range(CHUNKS):
        here = pl.ds(*dense_chunks[r])
        total = reduce_last(dense_part, dense_part_in, dred_send, dred_recv, dense_chunks[r], r)
        out_ref[here, :] = (base[here, :] + total).astype(BF16)

    sent(outgoing.at[pl.ds(0, far)], disp_send, disp_recv.at[0])
    sent(outgoing_near.at[:, 0], near_send.at[0], near_recv.at[0])
    sent(part_near.at[:, 0], near_send.at[1], near_recv.at[1])
    sent(arrived.at[pl.ds(0, n_cut - 1), pl.ds(2, far)], gath_send, gath_recv.at[0, 0, 0])
    for w in range(2):
        sent(weights[w].at[pl.ds(0, n_chip - 1), 0], ring_send.at[w], ring_recv.at[0, w, 0])
        sent(weights[w].at[:, 0], sib_send.at[w], sib_recv.at[w])
    sent(part.at[pl.ds(0, n_cut - 1), pl.ds(2, far)], red_send, red_recv.at[0, 0, 0])
    sent(result.at[pl.ds(2, far)], ret_send, ret_recv)
    sent(dense_part.at[pl.ds(0, n_cut - 1)], dred_send, dred_recv.at[0, 0, 0])


def local(tokens, route, gate_prob, norm_gain, dense_in, dense_out, expert_in, expert_out):
    n_exp = lax.axis_size("expert")
    n_cut = lax.axis_size("cuts")
    rows, width = tokens.shape
    share = width // n_cut
    hidden = expert_in.shape[2]
    cap = max(2, 3 * rows // (2 * n_exp))
    n_chip = n_exp // 2
    depth = dense_in.shape[0]
    half_y = n_cut // 2
    dims = (n_exp, n_cut, cap, rows, width, share, hidden)
    vmem = pl.BlockSpec(memory_space=pltpu.VMEM)
    hbm = pl.BlockSpec(memory_space=pl.ANY)
    dma = pltpu.SemaphoreType.DMA
    return pl.pallas_call(
        functools.partial(layer_kernel, dims),
        out_shape=jax.ShapeDtypeStruct((rows, share), BF16),
        in_specs=[hbm, vmem, vmem, vmem, hbm, hbm, hbm, hbm],
        out_specs=vmem,
        scratch_shapes=[
            pltpu.VMEM((rows, width), BF16),
            pltpu.VMEM((rows, width), BF16),
            pltpu.VMEM((n_exp * cap, rows), BF16),
            pltpu.VMEM((rows, n_exp * cap), BF16),
            pltpu.VMEM((rows, 128), F32),
            pltpu.VMEM((n_exp, cap, share), BF16),
            pltpu.VMEM((n_cut, 2, cap, share), BF16),
            pltpu.VMEM((n_cut, n_exp, cap, share), BF16),
            pltpu.VMEM((width, hidden), BF16),
            pltpu.VMEM((hidden, width), BF16),
            pltpu.VMEM((n_chip, 2, depth, hidden), BF16),
            pltpu.VMEM((n_chip, 2, hidden, depth), BF16),
            pltpu.VMEM((-(-n_exp // CHUNKS) * cap, hidden), BF16),
            pltpu.VMEM((n_cut, n_exp, cap, share), BF16),
            pltpu.VMEM((n_cut, 2, cap, share), BF16),
            pltpu.VMEM((2, half_y, n_exp, cap, share), BF16),
            pltpu.VMEM((n_cut, 2, cap, share), BF16),
            pltpu.VMEM((n_exp, cap, share), BF16),
            pltpu.VMEM((n_exp, cap, share), BF16),
            pltpu.VMEM((rows, hidden), BF16),
            pltpu.VMEM((n_cut, rows, share), BF16),
            pltpu.VMEM((2, half_y, rows, share), BF16),
            pltpu.VMEM((rows, share), F32),
            dma((5,)),
            dma((2,)),
            dma((2,)),
            dma,
            dma((CHUNKS,)),
            dma,
            dma((2, half_y, CHUNKS)),
            dma((2,)),
            dma((2, 2, n_chip // 2)),
            dma((2,)),
            dma((2,)),
            dma,
            dma((2, half_y, CHUNKS)),
            dma,
            dma,
            dma,
            dma((2, half_y, CHUNKS)),
        ],
        compiler_params=pltpu.CompilerParams(
            collective_id=0, has_side_effects=True, vmem_limit_bytes=60 * 1024 * 1024
        ),
        name="moe_layer",
    )(
        tokens,
        route.reshape(1, rows),
        gate_prob.reshape(1, rows),
        norm_gain.reshape(1, width),
        dense_in,
        dense_out,
        expert_in.reshape(width, hidden),
        expert_out.reshape(hidden, width),
    )


def solution(mesh):
    return jax.shard_map(
        local,
        mesh=mesh,
        in_specs=(
            P(("groups", "expert"), None),
            P(("groups", "expert"), None),
            P(("groups", "expert")),
            P(),
            P("expert", "cuts"),
            P("cuts", "expert"),
            P("expert", None, "cuts"),
            P("expert", "cuts", None),
        ),
        out_specs=P(("groups", "expert"), "cuts"),
        check_vma=False,
    )
```

```python
import functools

import jax
import jax.numpy as jnp
from jax import lax
from jax.experimental import pallas as pl
from jax.experimental.pallas import tpu as pltpu
from jax.sharding import PartitionSpec as P

MESH = pl.DeviceIdType.MESH
F32 = jnp.float32
BF16 = jnp.bfloat16
CHUNKS = 4


ORDER = (
    ("ring_own", 0), ("gather", 0, 0), ("gather", 0, 1), ("gather", 1, 0), ("gather", 0, 2),
    ("gather", 1, 1), ("gather", 0, 3), ("ring", 0, 0, 1), ("gather", 2, 0), ("ring", 0, 1, 1),
    ("gather", 1, 2), ("ring", 0, 0, 2), ("gather", 2, 1), ("gather", 1, 3), ("ring", 0, 1, 2),
    ("ring_own", 1), ("gather", 3, 0), ("gather", 2, 2), ("ring", 0, 0, 3), ("gather", 3, 1),
    ("ring", 0, 1, 3), ("gather", 2, 3), ("gather", 4, 0), ("expert", 0), ("ring", 1, 0, 1),
    ("gather", 3, 2), ("gather", 4, 1), ("expert", 1), ("gather", 3, 3), ("ered", 4, 1),
    ("gather", 4, 2), ("ring", 1, 1, 1), ("expert", 2), ("ring", 0, 0, 4), ("ring", 0, 1, 4),
    ("ered", 4, 2), ("gather", 4, 3), ("expert", 3), ("ered", 3, 1), ("ring", 1, 0, 2),
    ("ered", 4, 3), ("dfirst", 0), ("ered", 3, 2), ("ring", 1, 1, 2), ("dfirst", 1),
    ("ered", 2, 1), ("ered", 3, 3), ("ring", 1, 0, 3), ("ered", 2, 2), ("ring", 1, 1, 3),
    ("nrsend",), ("ered", 1, 1), ("ered", 2, 3), ("ring", 1, 0, 4), ("ered", 1, 2),
    ("ring", 1, 1, 4), ("home", 1), ("ered", 1, 3), ("dsecond", 0), ("dred", 4, 0),
    ("dred", 4, 1), ("dred", 4, 2), ("dred", 4, 3), ("home", 2), ("dsecond", 1), ("home", 3),
    ("dred", 3, 0), ("dsecond", 2), ("dred", 3, 1), ("dred", 3, 2), ("dred", 3, 3),
    ("dsecond", 3), ("dred", 2, 0), ("dred", 2, 1), ("base",), ("dred", 2, 2), ("dred", 2, 3),
    ("dred", 1, 0), ("dred", 1, 1), ("dred", 1, 2), ("dred", 1, 3), ("last", 0), ("last", 1),
    ("last", 2), ("last", 3),
)


def layer_kernel(
    dims,
    tokens_hbm,
    route_ref,
    gate_ref,
    gain_ref,
    dense_in_hbm,
    dense_out_hbm,
    expert_in_hbm,
    expert_out_hbm,
    out_ref,
    tok,
    norm,
    pick,
    pick_home,
    gate_wide,
    outgoing,
    outgoing_near,
    arrived,
    w_in,
    w_out,
    d_in,
    d_out,
    inner,
    part,
    part_near,
    part_in,
    near,
    result,
    returned,
    dense_act,
    dense_part,
    dense_part_in,
    base,
    near_home,
    load_sem,
    near_send,
    near_recv,
    disp_send,
    disp_recv,
    gath_send,
    gath_recv,
    ring_send,
    ring_recv,
    sib_send,
    sib_recv,
    red_send,
    red_recv,
    ret_send,
    ret_recv,
    dred_send,
    dred_recv,
    next_sem,
    next_recv,
):
    n_exp, n_cut, cap, rows, width, share, hidden = dims
    n_chip = n_exp // 2
    half_x, half_y = n_chip // 2, n_cut // 2
    offsets = [0] + [(p + 1) // 2 if p % 2 else -(p // 2) for p in range(1, n_chip)]
    far = n_exp - 2
    size = -(-far // CHUNKS)
    size += size % 2
    chunks = [(first, min(size, n_exp - first)) for first in range(2, n_exp, size)]
    dsize = rows // CHUNKS
    dense_chunks = [(first, dsize) for first in range(0, rows, dsize)]

    e = lax.axis_index("expert")
    c = lax.axis_index("cuts")
    x = e // 2
    core = e - 2 * x
    other = 1 - core
    sibling = {"expert": 2 * x + other}

    def chip(offset):
        return lax.rem(x + offset + n_chip, n_chip)

    def cut(offset):
        return lax.rem(c + offset + n_cut, n_cut)

    def ring_device(way):
        return {"expert": 2 * chip(1 if way == 0 else -1) + core}

    def cut_device(way):
        return {"cuts": cut(1 if way == 0 else -1)}

    def remote(src, dst, send_sem, recv_sem, device):
        return pltpu.make_async_remote_copy(
            src_ref=src,
            dst_ref=dst,
            send_sem=send_sem,
            recv_sem=recv_sem,
            device_id=device,
            device_id_type=MESH,
        )

    def send(src, dst, send_sem, recv_sem, device):
        remote(src, dst, send_sem, recv_sem, device).start()

    def arrive(dst, recv_sem, send_sem):
        remote(dst, dst, send_sem, recv_sem, sibling).wait_recv()

    def sent(src, send_sem, recv_sem):
        remote(src, src, send_sem, recv_sem, sibling).wait_send()

    def halves(chunk):
        first, count = chunk
        return (
            pl.ds(first, count // 2),
            pl.ds(first + count // 2, count // 2),
        )

    loads = [
        pltpu.make_async_copy(src, dst, load_sem.at[number])
        for number, (src, dst) in enumerate(
            (
                (tokens_hbm, tok),
                (expert_in_hbm, w_in),
                (expert_out_hbm, w_out),
                (dense_in_hbm, d_in.at[x, core]),
                (dense_out_hbm, d_out.at[x, core]),
            )
        )
    ]
    loads[0].start()

    barrier = pltpu.get_barrier_semaphore()
    for step in range(1, n_exp):
        pl.semaphore_signal(
            barrier, inc=1, device_id={"expert": lax.rem(e + step, n_exp)}, device_id_type=MESH
        )
    for way in range(2):
        pl.semaphore_signal(barrier, inc=1, device_id=cut_device(way), device_id_type=MESH)

    route = route_ref[...]
    hot = lax.broadcasted_iota(jnp.int32, (n_exp, rows), 0) == route
    hot = jnp.where(hot, 1.0, 0.0).astype(F32)
    earlier = lax.broadcasted_iota(jnp.int32, (rows, rows), 0) < lax.broadcasted_iota(
        jnp.int32, (rows, rows), 1
    )
    earlier = jnp.where(earlier, 1.0, 0.0).astype(BF16)
    before = jnp.dot(hot.astype(BF16), earlier, preferred_element_type=F32)
    position = jnp.sum(before * hot, axis=0, keepdims=True)
    target = route * cap + position.astype(jnp.int32)
    slots = lax.broadcasted_iota(jnp.int32, (n_exp * cap, rows), 0)
    pick[...] = jnp.where(slots == target, 1.0, 0.0).astype(BF16)

    loads[0].wait()
    for number in (3, 4, 1, 2):
        loads[number].start()
    block = rows // 8

    @pl.loop(0, 8)
    def _(i):
        here = pl.ds(pl.multiple_of(i * block, block), block)
        wide = tok[here, :].astype(F32)
        meansq = jnp.mean(wide * wide, axis=-1, keepdims=True)
        norm[here, :] = (wide * lax.rsqrt(meansq + 1e-06) * gain_ref[...]).astype(BF16)

    own_columns = pl.ds(pl.multiple_of(c * share, share), share)
    outgoing[...] = (
        jnp.dot(pick[...], norm[:, own_columns], preferred_element_type=F32)
        .astype(BF16)
        .reshape(n_exp, cap, share)
    )
    pl.semaphore_wait(barrier, n_exp + 1)

    def chunk_of(slot):
        return (slot - 2) // size

    for p in range(1, n_chip):
        for k in range(2):
            to = 2 * chip(-offsets[p]) + k
            send(
                outgoing.at[to],
                arrived.at[c, 2 * p + core],
                disp_send,
                disp_recv.at[chunk_of(2 * p)],
                {"expert": to},
            )

    near_rows = pick[pl.ds(pl.multiple_of(2 * x * cap, 2 * cap), 2 * cap), :]
    for k in range(n_cut):
        outgoing_near[k] = (
            jnp.dot(near_rows, norm[:, pl.ds(k * share, share)], preferred_element_type=F32)
            .astype(BF16)
            .reshape(2, cap, share)
        )
    send(
        outgoing_near.at[:, other], arrived.at[:, core], near_send.at[0], near_recv.at[0], sibling
    )
    for k in range(n_cut):
        arrived[k, core] = outgoing_near[k, core]

    weights = (d_in, d_out)

    def ring_piece(w, origin, p):
        half = weights[w].shape[2] // 2
        return weights[w].at[origin, core, pl.ds(p * half, half)]

    def ring_own(w):
        loads[3 + w].wait()
        for p in range(2):
            piece = ring_piece(w, x, p)
            for way in range(2):
                send(piece, piece, ring_send.at[w], ring_recv.at[way, w, p, 0], ring_device(way))
        own = weights[w].at[x, core]
        send(own, own, sib_send.at[w], sib_recv.at[w], sibling)

    def ring_event(w, p, hop):
        for way in range(2):
            if hop == half_x and p != way:
                continue
            piece = ring_piece(w, chip(-hop if way == 0 else hop), p)
            arrive(piece, ring_recv.at[way, w, p, hop - 1], ring_send.at[w])
            if hop < half_x - 1 or (hop == half_x - 1 and p == way):
                send(piece, piece, ring_send.at[w], ring_recv.at[way, w, p, hop], ring_device(way))
            send(piece, piece, sib_send.at[w], sib_recv.at[w], sibling)

    def gather_event(hop, r):
        first, count = chunks[r]
        whole = pl.ds(first, count)
        if hop == 0:
            arrive(arrived.at[c, whole], disp_recv.at[r], disp_send)
        for way in range(2):
            here = halves(chunks[r])[way] if hop == half_y else whole
            onward = halves(chunks[r])[way] if hop == half_y - 1 else here
            origin = cut(-hop if way == 0 else hop)
            if hop > 0:
                arrive(arrived.at[origin, here], gath_recv.at[way, hop - 1, r], gath_send)
            if hop < half_y:
                piece = arrived.at[origin, onward]
                send(piece, piece, gath_send, gath_recv.at[way, hop, r], cut_device(way))

    def expert_rows(first, count, keep):
        flat = jnp.concatenate(
            [
                arrived[k, pl.ds(first, count)].reshape(count * cap, share)
                for k in range(n_cut)
            ],
            axis=1,
        )
        for n in range(2):
            columns = pl.ds(n * (hidden // 2), hidden // 2)
            inner[pl.ds(0, count * cap), columns] = jax.nn.gelu(
                jnp.dot(flat, w_in[:, columns], preferred_element_type=F32)
            ).astype(BF16)
        for k in range(0, n_cut, 2):
            both = jnp.dot(
                inner[pl.ds(0, count * cap), :],
                w_out[:, pl.ds(k * share, 2 * share)],
                preferred_element_type=F32,
            ).astype(BF16)
            for j in range(2):
                keep(k + j, both[:, j * share : (j + 1) * share].reshape(count, cap, share))

    def expert_near():
        def keep(k, values):
            part_near[k] = values

        arrive(arrived.at[:, other], near_recv.at[0], near_send.at[0])
        expert_rows(0, 2, keep)
        send(
            part_near.at[:, other], near.at[:, core], near_send.at[1], near_recv.at[1], sibling
        )
        for k in range(n_cut):
            near[k, core] = part_near[k, core]

    pairs = [(half_y, half_y - 1)]
    pairs += [(-step, step - 1) for step in range(half_y - 1, 0, -1)]

    def next_send():
        for i, pair in enumerate(pairs):
            for offset in pair:
                k = cut(offset)
                for slot in range(2, 6):
                    to = 2 * chip(offsets[slot // 2]) + slot % 2
                    place = slot // 2 * 2 + core
                    send(
                        part.at[k, slot],
                        near.at[k, place],
                        next_sem,
                        next_recv.at[i],
                        {"expert": to},
                    )

    def expert_chunk(r):
        first, count = chunks[r]

        def keep(k, values):
            part[k, pl.ds(first, count)] = values

        expert_rows(first, count, keep)

    def reduce_event(own, landed, send_sem, recv_sem, chunk, step, r):
        whole = pl.ds(*chunk)
        for way in range(2):
            half, rest = halves(chunk)[way], halves(chunk)[1 - way]
            home = cut(step if way == 0 else -step)
            to = step - 1
            if step == half_y:
                send(
                    own.at[home, half],
                    landed.at[way, to, half],
                    send_sem,
                    recv_sem.at[way, to, r],
                    cut_device(way),
                )
                continue
            here = half if step == half_y - 1 else whole
            arrive(landed.at[way, step, here], recv_sem.at[way, step, r], send_sem)
            landed[way, step, here] = (
                landed[way, step, here].astype(F32) + own[home, here].astype(F32)
            ).astype(BF16)
            if step == half_y - 1:
                landed[way, step, rest] = own[home, rest]
            send(
                landed.at[way, step, whole],
                landed.at[way, to, whole],
                send_sem,
                recv_sem.at[way, to, r],
                cut_device(way),
            )

    def reduce_last(own, landed, send_sem, recv_sem, chunk, r):
        whole = pl.ds(*chunk)
        total = own[c, whole].astype(F32)
        for way in range(2):
            arrive(landed.at[way, 0, whole], recv_sem.at[way, 0, r], send_sem)
            total = total + landed[way, 0, whole].astype(F32)
        return total

    def expert_reduce(step, r):
        reduce_event(part, part_in, red_send, red_recv, chunks[r], step, r)

    def go_home(r):
        first, count = chunks[r]
        result[pl.ds(first, count)] = reduce_last(
            part, part_in, red_send, red_recv, chunks[r], r
        ).astype(BF16)
        for slot in range(first, first + count):
            to = 2 * chip(offsets[slot // 2]) + slot % 2
            send(result.at[slot], returned.at[e], ret_send, ret_recv, {"expert": to})

    def dense_first(n):
        if n == 0:
            arrive(d_in.at[:, other], sib_recv.at[0], sib_send.at[0])
        columns = pl.ds(n * (hidden // 2), hidden // 2)
        dense_act[:, columns] = jax.nn.gelu(
            jnp.dot(
                norm[...],
                d_in[:, :, :, columns].reshape(width, hidden // 2),
                preferred_element_type=F32,
            )
        ).astype(BF16)

    def dense_second(i):
        if i == 0:
            arrive(d_out.at[:, other], sib_recv.at[1], sib_send.at[1])
            arrive(near.at[:, other], near_recv.at[1], near_send.at[1])
        arrive(near.at[pl.ds(0, 2), pl.ds(2, 4)], next_recv.at[i], next_sem)
        ks = [cut(offset) for offset in pairs[i]]
        both = jnp.dot(
            dense_act[...],
            jnp.concatenate([d_out[k, j] for k in ks for j in range(2)], axis=1),
            preferred_element_type=F32,
        )
        rows_near = jnp.concatenate([near[k].reshape(6 * cap, share) for k in ks], axis=1)
        both = both + gate_wide[:, 0:1] * jnp.dot(
            near_home[...], rows_near, preferred_element_type=F32
        )
        both = both.astype(BF16)
        dense_part[ks[0]] = both[:, :share]
        dense_part[ks[1]] = both[:, share:]

    def dense_reduce(step, r):
        reduce_event(
            dense_part, dense_part_in, dred_send, dred_recv, dense_chunks[r], step, r
        )

    def home_tables():
        gate_wide[...] = jnp.transpose(jnp.broadcast_to(gate_ref[...], (128, rows)))
        wide = jnp.transpose(jnp.broadcast_to(target.astype(F32), (128, rows)))[:, 0:1]
        slot_of = lax.broadcasted_iota(jnp.int32, (rows, n_exp * cap), 1).astype(F32)
        pick_home[...] = jnp.where(slot_of == wide, 1.0, 0.0).astype(BF16)
        lane = lax.broadcasted_iota(jnp.int32, (rows, 6 * cap), 1)
        first = jnp.where(
            lane < 2 * cap,
            2 * cap * x,
            jnp.where(
                lane < 4 * cap, 2 * cap * (chip(-1) - 1), 2 * cap * (chip(1) - 2)
            ),
        )
        near_home[...] = jnp.where((lane + first).astype(F32) == wide, 1.0, 0.0).astype(BF16)

    def dense_base():
        arrive(returned.at[pl.ds(0, far - 4)], ret_recv, ret_send)
        expert_res = jnp.dot(
            pick_home[...],
            returned[...].reshape(n_exp * cap, share),
            preferred_element_type=F32,
        )
        base[...] = tok[:, own_columns].astype(F32) + gate_wide[:, 0:1] * expert_res

    def dense_last(r):
        here = pl.ds(*dense_chunks[r])
        total = reduce_last(dense_part, dense_part_in, dred_send, dred_recv, dense_chunks[r], r)
        out_ref[here, :] = (base[here, :] + total).astype(BF16)

    for offset in (-1, 0, 1):
        returned[pl.ds(2 * chip(offset), 2)] = jnp.zeros((2, cap, share), BF16)

    ring_own(0)
    home_tables()
    loads[1].wait()
    loads[2].wait()
    expert_near()
    steps = {
        "gather": gather_event,
        "ring_own": ring_own,
        "ring": ring_event,
        "expert": expert_chunk,
        "nrsend": next_send,
        "ered": expert_reduce,
        "home": go_home,
        "dfirst": dense_first,
        "dsecond": dense_second,
        "dred": dense_reduce,
        "base": dense_base,
        "last": dense_last,
    }
    for name, *where in ORDER:
        if (name, *where) != ("ring_own", 0):
            steps[name](*where)

    sent(outgoing.at[pl.ds(0, far)], disp_send, disp_recv.at[0])
    sent(outgoing_near.at[:, 0], near_send.at[0], near_recv.at[0])
    sent(part_near.at[:, 0], near_send.at[1], near_recv.at[1])
    sent(arrived.at[pl.ds(0, n_cut - 1), pl.ds(2, far)], gath_send, gath_recv.at[0, 0, 0])
    for w in range(2):
        sent(weights[w].at[pl.ds(0, n_chip - 1), 0], ring_send.at[w], ring_recv.at[0, w, 0, 0])
        sent(weights[w].at[:, 0], sib_send.at[w], sib_recv.at[w])
    sent(part.at[:, pl.ds(2, 4)], next_sem, next_recv.at[0])
    sent(part.at[pl.ds(0, n_cut - 1), pl.ds(6, far - 4)], red_send, red_recv.at[0, 0, 0])
    sent(result.at[pl.ds(6, far - 4)], ret_send, ret_recv)
    sent(dense_part.at[pl.ds(0, n_cut - 1)], dred_send, dred_recv.at[0, 0, 0])


def local(tokens, route, gate_prob, norm_gain, dense_in, dense_out, expert_in, expert_out):
    n_exp = lax.axis_size("expert")
    n_cut = lax.axis_size("cuts")
    rows, width = tokens.shape
    share = width // n_cut
    hidden = expert_in.shape[2]
    cap = max(2, 3 * rows // (2 * n_exp))
    n_chip = n_exp // 2
    depth = dense_in.shape[0]
    half_y = n_cut // 2
    dims = (n_exp, n_cut, cap, rows, width, share, hidden)
    vmem = pl.BlockSpec(memory_space=pltpu.VMEM)
    hbm = pl.BlockSpec(memory_space=pltpu.HBM)
    dma = pltpu.SemaphoreType.DMA
    return pl.pallas_call(
        functools.partial(layer_kernel, dims),
        out_shape=jax.ShapeDtypeStruct((rows, share), BF16),
        in_specs=[hbm, vmem, vmem, vmem, hbm, hbm, hbm, hbm],
        out_specs=vmem,
        scratch_shapes=[
            pltpu.VMEM((rows, width), BF16),
            pltpu.VMEM((rows, width), BF16),
            pltpu.VMEM((n_exp * cap, rows), BF16),
            pltpu.VMEM((rows, n_exp * cap), BF16),
            pltpu.VMEM((rows, 128), F32),
            pltpu.VMEM((n_exp, cap, share), BF16),
            pltpu.VMEM((n_cut, 2, cap, share), BF16),
            pltpu.VMEM((n_cut, n_exp, cap, share), BF16),
            pltpu.VMEM((width, hidden), BF16),
            pltpu.VMEM((hidden, width), BF16),
            pltpu.VMEM((n_chip, 2, depth, hidden), BF16),
            pltpu.VMEM((n_chip, 2, hidden, depth), BF16),
            pltpu.VMEM((-(-n_exp // CHUNKS) * cap, hidden), BF16),
            pltpu.VMEM((n_cut, n_exp, cap, share), BF16),
            pltpu.VMEM((n_cut, 2, cap, share), BF16),
            pltpu.VMEM((2, half_y, n_exp, cap, share), BF16),
            pltpu.VMEM((n_cut, 6, cap, share), BF16),
            pltpu.VMEM((n_exp, cap, share), BF16),
            pltpu.VMEM((n_exp, cap, share), BF16),
            pltpu.VMEM((rows, hidden), BF16),
            pltpu.VMEM((n_cut, rows, share), BF16),
            pltpu.VMEM((2, half_y, rows, share), BF16),
            pltpu.VMEM((rows, share), F32),
            pltpu.VMEM((rows, 6 * cap), BF16),
            dma((5,)),
            dma((2,)),
            dma((2,)),
            dma,
            dma((CHUNKS,)),
            dma,
            dma((2, half_y, CHUNKS)),
            dma((2,)),
            dma((2, 2, 2, n_chip // 2)),
            dma((2,)),
            dma((2,)),
            dma,
            dma((2, half_y, CHUNKS)),
            dma,
            dma,
            dma,
            dma((2, half_y, CHUNKS)),
            dma,
            dma((half_y,)),
        ],
        compiler_params=pltpu.CompilerParams(
            collective_id=0, has_side_effects=True, vmem_limit_bytes=52 * 1024 * 1024
        ),
        name="moe_layer",
    )(
        *(
            pltpu.with_memory_space_constraint(operand, pltpu.HBM)
            for operand in (
                tokens,
                route.reshape(1, rows),
                gate_prob.reshape(1, rows),
                norm_gain.reshape(1, width),
                dense_in,
                dense_out,
                expert_in.reshape(width, hidden),
                expert_out.reshape(hidden, width),
            )
        )
    )


def solution(mesh):
    return jax.shard_map(
        local,
        mesh=mesh,
        in_specs=(
            P(("groups", "expert"), None),
            P(("groups", "expert"), None),
            P(("groups", "expert")),
            P(),
            P("expert", "cuts"),
            P("cuts", "expert"),
            P("expert", None, "cuts"),
            P("expert", "cuts", None),
        ),
        out_specs=P(("groups", "expert"), "cuts"),
        check_vma=False,
    )
```

```python
import functools

import jax
import jax.numpy as jnp
from jax import lax
from jax.experimental import pallas as pl
from jax.experimental.pallas import tpu as pltpu
from jax.sharding import PartitionSpec as P

MESH = pl.DeviceIdType.MESH
F32 = jnp.float32
BF16 = jnp.bfloat16
CHUNKS = 4
BLOCKS = 4


ORDER = (
    ("ring_own", 0), ("gather", 0, 0), ("gather", 0, 1), ("gather", 1, 0), ("gather", 0, 2),
    ("gather", 1, 1), ("gather", 0, 3), ("ring", 0, 0, 1), ("gather", 2, 0), ("ring", 0, 1, 1),
    ("gather", 1, 2), ("ring", 0, 0, 2), ("gather", 2, 1), ("gather", 1, 3), ("ring", 0, 1, 2),
    ("ring_own", 1), ("gather", 3, 0), ("gather", 2, 2), ("ring", 0, 0, 3), ("gather", 3, 1),
    ("ring", 0, 1, 3), ("gather", 2, 3), ("gather", 4, 0), ("expert", 0), ("ring", 1, 0, 1),
    ("gather", 3, 2), ("gather", 4, 1), ("expert", 1), ("gather", 3, 3), ("ered", 4, 1),
    ("gather", 4, 2), ("ring", 1, 1, 1), ("expert", 2), ("ring", 0, 0, 4), ("ring", 0, 1, 4),
    ("ered", 4, 2), ("gather", 4, 3), ("expert", 3), ("ered", 3, 1), ("ring", 1, 0, 2),
    ("ered", 4, 3), ("dfirst", 0), ("ered", 3, 2), ("ring", 1, 1, 2), ("dfirst", 1),
    ("ered", 2, 1), ("ered", 3, 3), ("ring", 1, 0, 3), ("ered", 2, 2), ("ring", 1, 1, 3),
    ("nrsend",), ("ered", 1, 1), ("ered", 2, 3), ("ring", 1, 0, 4), ("ered", 1, 2),
    ("ring", 1, 1, 4), ("home", 1), ("ered", 1, 3), ("dsecond", 0), ("dred", 4, 0),
    ("dred", 4, 1), ("dred", 4, 2), ("dred", 4, 3), ("home", 2), ("dsecond", 1), ("home", 3),
    ("dred", 3, 0), ("dsecond", 2), ("dred", 3, 1), ("dred", 3, 2), ("dred", 3, 3),
    ("dsecond", 3), ("dred", 2, 0), ("dred", 2, 1), ("base",), ("dred", 2, 2), ("dred", 2, 3),
    ("dred", 1, 0), ("dred", 1, 1), ("dred", 1, 2), ("dred", 1, 3), ("last", 0), ("last", 1),
    ("last", 2), ("last", 3),
)


def layer_kernel(
    dims,
    tokens_hbm,
    route_hbm,
    gate_hbm,
    gain_hbm,
    dense_in_hbm,
    dense_out_hbm,
    expert_in_hbm,
    expert_out_hbm,
    out_ref,
    route_ref,
    gate_ref,
    gain_ref,
    scale,
    tok,
    norm,
    pick,
    pick_home,
    gate_wide,
    outgoing,
    outgoing_near,
    arrived,
    w_in,
    w_out,
    d_in,
    d_out,
    inner,
    part,
    part_near,
    part_in,
    near,
    result,
    returned,
    dense_act,
    dense_part,
    dense_part_in,
    base,
    near_home,
    load_sem,
    near_send,
    near_recv,
    disp_send,
    disp_recv,
    gath_send,
    gath_recv,
    ring_send,
    ring_recv,
    sib_send,
    sib_recv,
    red_send,
    red_recv,
    ret_send,
    ret_recv,
    dred_send,
    dred_recv,
    next_sem,
    next_recv,
):
    n_exp, n_cut, cap, rows, width, share, hidden = dims
    n_chip = n_exp // 2
    half_x, half_y = n_chip // 2, n_cut // 2
    offsets = [0] + [(p + 1) // 2 if p % 2 else -(p // 2) for p in range(1, n_chip)]
    far = n_exp - 2
    size = -(-far // CHUNKS)
    size += size % 2
    chunks = [(first, min(size, n_exp - first)) for first in range(2, n_exp, size)]
    dsize = rows // CHUNKS
    dense_chunks = [(first, dsize) for first in range(0, rows, dsize)]

    e = lax.axis_index("expert")
    c = lax.axis_index("cuts")
    x = e // 2
    core = e - 2 * x
    other = 1 - core
    sibling = {"expert": 2 * x + other}

    def chip(offset):
        return lax.rem(x + offset + n_chip, n_chip)

    def cut(offset):
        return lax.rem(c + offset + n_cut, n_cut)

    def ring_device(way):
        return {"expert": 2 * chip(1 if way == 0 else -1) + core}

    def cut_device(way):
        return {"cuts": cut(1 if way == 0 else -1)}

    def remote(src, dst, send_sem, recv_sem, device):
        return pltpu.make_async_remote_copy(
            src_ref=src,
            dst_ref=dst,
            send_sem=send_sem,
            recv_sem=recv_sem,
            device_id=device,
            device_id_type=MESH,
        )

    def send(src, dst, send_sem, recv_sem, device):
        remote(src, dst, send_sem, recv_sem, device).start()

    def arrive(dst, recv_sem, send_sem):
        remote(dst, dst, send_sem, recv_sem, sibling).wait_recv()

    def sent(src, send_sem, recv_sem):
        remote(src, src, send_sem, recv_sem, sibling).wait_send()

    def halves(chunk):
        first, count = chunk
        return (
            pl.ds(first, count // 2),
            pl.ds(first + count // 2, count // 2),
        )

    block = rows // BLOCKS
    blocks = [pl.ds(n * block, block) for n in range(BLOCKS)]
    copies = [
        (expert_in_hbm, w_in),
        (expert_out_hbm, w_out),
        (dense_in_hbm, d_in.at[x, core]),
        (dense_out_hbm, d_out.at[x, core]),
        (route_hbm, route_ref),
        (gain_hbm, gain_ref),
        (gate_hbm, gate_ref),
    ]
    copies += [(tokens_hbm.at[here], tok.at[here]) for here in blocks]
    loads = [
        pltpu.make_async_copy(src, dst, load_sem.at[number])
        for number, (src, dst) in enumerate(copies)
    ]
    for copy in loads[4:]:
        copy.start()

    barrier = pltpu.get_barrier_semaphore()
    for step in range(1, n_exp):
        pl.semaphore_signal(
            barrier, inc=1, device_id={"expert": lax.rem(e + step, n_exp)}, device_id_type=MESH
        )
    for way in range(2):
        pl.semaphore_signal(barrier, inc=1, device_id=cut_device(way), device_id_type=MESH)

    loads[4].wait()
    route = route_ref[...]
    hot = lax.broadcasted_iota(jnp.int32, (n_exp, rows), 0) == route
    hot = jnp.where(hot, 1.0, 0.0).astype(F32)
    earlier = lax.broadcasted_iota(jnp.int32, (rows, rows), 0) < lax.broadcasted_iota(
        jnp.int32, (rows, rows), 1
    )
    earlier = jnp.where(earlier, 1.0, 0.0).astype(BF16)
    before = jnp.dot(hot.astype(BF16), earlier, preferred_element_type=F32)
    position = jnp.sum(before * hot, axis=0, keepdims=True)
    target = route * cap + position.astype(jnp.int32)
    slots = lax.broadcasted_iota(jnp.int32, (n_exp * cap, rows), 0)
    pick[...] = jnp.where(slots == target, 1.0, 0.0).astype(BF16)

    own_columns = pl.ds(pl.multiple_of(c * share, share), share)
    loads[5].wait()
    for n, here in enumerate(blocks):
        loads[7 + n].wait()
        wide = tok[here, :].astype(F32)
        factor = lax.rsqrt(jnp.mean(wide * wide, axis=-1, keepdims=True) + 1e-06)
        scale[here, :] = jnp.broadcast_to(factor, (block, 128))
        norm[here, own_columns] = (
            tok[here, own_columns].astype(F32) * factor * gain_ref[:, own_columns]
        ).astype(BF16)
    for number in (2, 3, 0, 1):
        loads[number].start()
    outgoing[...] = (
        jnp.dot(pick[...], norm[:, own_columns], preferred_element_type=F32)
        .astype(BF16)
        .reshape(n_exp, cap, share)
    )
    pl.semaphore_wait(barrier, n_exp + 1)

    def chunk_of(slot):
        return (slot - 2) // size

    for p in range(1, n_chip):
        for k in range(2):
            to = 2 * chip(-offsets[p]) + k
            send(
                outgoing.at[to],
                arrived.at[c, 2 * p + core],
                disp_send,
                disp_recv.at[chunk_of(2 * p)],
                {"expert": to},
            )

    @pl.loop(0, 8)
    def _(n):
        here = pl.ds(pl.multiple_of(n * (rows // 8), rows // 8), rows // 8)
        wide = tok[here, :].astype(F32)
        norm[here, :] = (wide * scale[here, 0:1] * gain_ref[...]).astype(BF16)

    near_rows = pick[pl.ds(pl.multiple_of(2 * x * cap, 2 * cap), 2 * cap), :]
    for k in range(n_cut):
        outgoing_near[k] = (
            jnp.dot(near_rows, norm[:, pl.ds(k * share, share)], preferred_element_type=F32)
            .astype(BF16)
            .reshape(2, cap, share)
        )
    send(
        outgoing_near.at[:, other], arrived.at[:, core], near_send.at[0], near_recv.at[0], sibling
    )
    for k in range(n_cut):
        arrived[k, core] = outgoing_near[k, core]

    weights = (d_in, d_out)

    def ring_piece(w, origin, p):
        half = weights[w].shape[2] // 2
        return weights[w].at[origin, core, pl.ds(p * half, half)]

    def ring_own(w):
        loads[2 + w].wait()
        for p in range(2):
            piece = ring_piece(w, x, p)
            for way in range(2):
                send(piece, piece, ring_send.at[w], ring_recv.at[way, w, p, 0], ring_device(way))
        own = weights[w].at[x, core]
        send(own, own, sib_send.at[w], sib_recv.at[w], sibling)

    def ring_event(w, p, hop):
        for way in range(2):
            if hop == half_x and p != way:
                continue
            piece = ring_piece(w, chip(-hop if way == 0 else hop), p)
            arrive(piece, ring_recv.at[way, w, p, hop - 1], ring_send.at[w])
            if hop < half_x - 1 or (hop == half_x - 1 and p == way):
                send(piece, piece, ring_send.at[w], ring_recv.at[way, w, p, hop], ring_device(way))
            send(piece, piece, sib_send.at[w], sib_recv.at[w], sibling)

    def gather_event(hop, r):
        first, count = chunks[r]
        whole = pl.ds(first, count)
        if hop == 0:
            arrive(arrived.at[c, whole], disp_recv.at[r], disp_send)
        for way in range(2):
            here = halves(chunks[r])[way] if hop == half_y else whole
            onward = halves(chunks[r])[way] if hop == half_y - 1 else here
            origin = cut(-hop if way == 0 else hop)
            if hop > 0:
                arrive(arrived.at[origin, here], gath_recv.at[way, hop - 1, r], gath_send)
            if hop < half_y:
                piece = arrived.at[origin, onward]
                send(piece, piece, gath_send, gath_recv.at[way, hop, r], cut_device(way))

    def expert_rows(first, count, keep):
        flat = jnp.concatenate(
            [
                arrived[k, pl.ds(first, count)].reshape(count * cap, share)
                for k in range(n_cut)
            ],
            axis=1,
        )
        for n in range(2):
            columns = pl.ds(n * (hidden // 2), hidden // 2)
            inner[pl.ds(0, count * cap), columns] = jax.nn.gelu(
                jnp.dot(flat, w_in[:, columns], preferred_element_type=F32)
            ).astype(BF16)
        for k in range(0, n_cut, 2):
            both = jnp.dot(
                inner[pl.ds(0, count * cap), :],
                w_out[:, pl.ds(k * share, 2 * share)],
                preferred_element_type=F32,
            ).astype(BF16)
            for j in range(2):
                keep(k + j, both[:, j * share : (j + 1) * share].reshape(count, cap, share))

    def expert_near():
        def keep(k, values):
            part_near[k] = values

        arrive(arrived.at[:, other], near_recv.at[0], near_send.at[0])
        expert_rows(0, 2, keep)
        send(
            part_near.at[:, other], near.at[:, core], near_send.at[1], near_recv.at[1], sibling
        )
        for k in range(n_cut):
            near[k, core] = part_near[k, core]

    pairs = [(half_y, half_y - 1)]
    pairs += [(-step, step - 1) for step in range(half_y - 1, 0, -1)]

    def next_send():
        for i, pair in enumerate(pairs):
            for offset in pair:
                k = cut(offset)
                for slot in range(2, 6):
                    to = 2 * chip(offsets[slot // 2]) + slot % 2
                    place = slot // 2 * 2 + core
                    send(
                        part.at[k, slot],
                        near.at[k, place],
                        next_sem,
                        next_recv.at[i],
                        {"expert": to},
                    )

    def expert_chunk(r):
        first, count = chunks[r]

        def keep(k, values):
            part[k, pl.ds(first, count)] = values

        expert_rows(first, count, keep)

    def reduce_event(own, landed, send_sem, recv_sem, chunk, step, r):
        whole = pl.ds(*chunk)
        for way in range(2):
            half, rest = halves(chunk)[way], halves(chunk)[1 - way]
            home = cut(step if way == 0 else -step)
            to = step - 1
            if step == half_y:
                send(
                    own.at[home, half],
                    landed.at[way, to, half],
                    send_sem,
                    recv_sem.at[way, to, r],
                    cut_device(way),
                )
                continue
            here = half if step == half_y - 1 else whole
            arrive(landed.at[way, step, here], recv_sem.at[way, step, r], send_sem)
            landed[way, step, here] = (
                landed[way, step, here].astype(F32) + own[home, here].astype(F32)
            ).astype(BF16)
            if step == half_y - 1:
                landed[way, step, rest] = own[home, rest]
            send(
                landed.at[way, step, whole],
                landed.at[way, to, whole],
                send_sem,
                recv_sem.at[way, to, r],
                cut_device(way),
            )

    def reduce_last(own, landed, send_sem, recv_sem, chunk, r):
        whole = pl.ds(*chunk)
        total = own[c, whole].astype(F32)
        for way in range(2):
            arrive(landed.at[way, 0, whole], recv_sem.at[way, 0, r], send_sem)
            total = total + landed[way, 0, whole].astype(F32)
        return total

    def expert_reduce(step, r):
        reduce_event(part, part_in, red_send, red_recv, chunks[r], step, r)

    def go_home(r):
        first, count = chunks[r]
        result[pl.ds(first, count)] = reduce_last(
            part, part_in, red_send, red_recv, chunks[r], r
        ).astype(BF16)
        for slot in range(first, first + count):
            to = 2 * chip(offsets[slot // 2]) + slot % 2
            send(result.at[slot], returned.at[e], ret_send, ret_recv, {"expert": to})

    def dense_first(n):
        if n == 0:
            arrive(d_in.at[:, other], sib_recv.at[0], sib_send.at[0])
        columns = pl.ds(n * (hidden // 2), hidden // 2)
        dense_act[:, columns] = jax.nn.gelu(
            jnp.dot(
                norm[...],
                d_in[:, :, :, columns].reshape(width, hidden // 2),
                preferred_element_type=F32,
            )
        ).astype(BF16)

    def dense_second(i):
        if i == 0:
            arrive(d_out.at[:, other], sib_recv.at[1], sib_send.at[1])
            arrive(near.at[:, other], near_recv.at[1], near_send.at[1])
        arrive(near.at[pl.ds(0, 2), pl.ds(2, 4)], next_recv.at[i], next_sem)
        ks = [cut(offset) for offset in pairs[i]]
        both = jnp.dot(
            dense_act[...],
            jnp.concatenate([d_out[k, j] for k in ks for j in range(2)], axis=1),
            preferred_element_type=F32,
        )
        rows_near = jnp.concatenate([near[k].reshape(6 * cap, share) for k in ks], axis=1)
        both = both + gate_wide[:, 0:1] * jnp.dot(
            near_home[...], rows_near, preferred_element_type=F32
        )
        both = both.astype(BF16)
        dense_part[ks[0]] = both[:, :share]
        dense_part[ks[1]] = both[:, share:]

    def dense_reduce(step, r):
        reduce_event(
            dense_part, dense_part_in, dred_send, dred_recv, dense_chunks[r], step, r
        )

    def home_tables():
        gate_wide[...] = jnp.transpose(jnp.broadcast_to(gate_ref[...], (128, rows)))
        wide = jnp.transpose(jnp.broadcast_to(target.astype(F32), (128, rows)))[:, 0:1]
        slot_of = lax.broadcasted_iota(jnp.int32, (rows, n_exp * cap), 1).astype(F32)
        pick_home[...] = jnp.where(slot_of == wide, 1.0, 0.0).astype(BF16)
        lane = lax.broadcasted_iota(jnp.int32, (rows, 6 * cap), 1)
        first = jnp.where(
            lane < 2 * cap,
            2 * cap * x,
            jnp.where(
                lane < 4 * cap, 2 * cap * (chip(-1) - 1), 2 * cap * (chip(1) - 2)
            ),
        )
        near_home[...] = jnp.where((lane + first).astype(F32) == wide, 1.0, 0.0).astype(BF16)

    def dense_base():
        arrive(returned.at[pl.ds(0, far - 4)], ret_recv, ret_send)
        expert_res = jnp.dot(
            pick_home[...],
            returned[...].reshape(n_exp * cap, share),
            preferred_element_type=F32,
        )
        base[...] = tok[:, own_columns].astype(F32) + gate_wide[:, 0:1] * expert_res

    def dense_last(r):
        here = pl.ds(*dense_chunks[r])
        total = reduce_last(dense_part, dense_part_in, dred_send, dred_recv, dense_chunks[r], r)
        out_ref[here, :] = (base[here, :] + total).astype(BF16)

    for offset in (-1, 0, 1):
        returned[pl.ds(2 * chip(offset), 2)] = jnp.zeros((2, cap, share), BF16)

    ring_own(0)
    loads[6].wait()
    home_tables()
    loads[0].wait()
    loads[1].wait()
    expert_near()
    steps = {
        "gather": gather_event,
        "ring_own": ring_own,
        "ring": ring_event,
        "expert": expert_chunk,
        "nrsend": next_send,
        "ered": expert_reduce,
        "home": go_home,
        "dfirst": dense_first,
        "dsecond": dense_second,
        "dred": dense_reduce,
        "base": dense_base,
        "last": dense_last,
    }
    for name, *where in ORDER:
        if (name, *where) != ("ring_own", 0):
            steps[name](*where)

    sent(outgoing.at[pl.ds(0, far)], disp_send, disp_recv.at[0])
    sent(outgoing_near.at[:, 0], near_send.at[0], near_recv.at[0])
    sent(part_near.at[:, 0], near_send.at[1], near_recv.at[1])
    sent(arrived.at[pl.ds(0, n_cut - 1), pl.ds(2, far)], gath_send, gath_recv.at[0, 0, 0])
    for w in range(2):
        sent(weights[w].at[pl.ds(0, n_chip - 1), 0], ring_send.at[w], ring_recv.at[0, w, 0, 0])
        sent(weights[w].at[:, 0], sib_send.at[w], sib_recv.at[w])
    sent(part.at[:, pl.ds(2, 4)], next_sem, next_recv.at[0])
    sent(part.at[pl.ds(0, n_cut - 1), pl.ds(6, far - 4)], red_send, red_recv.at[0, 0, 0])
    sent(result.at[pl.ds(6, far - 4)], ret_send, ret_recv)
    sent(dense_part.at[pl.ds(0, n_cut - 1)], dred_send, dred_recv.at[0, 0, 0])


def local(tokens, route, gate_prob, norm_gain, dense_in, dense_out, expert_in, expert_out):
    n_exp = lax.axis_size("expert")
    n_cut = lax.axis_size("cuts")
    rows, width = tokens.shape
    share = width // n_cut
    hidden = expert_in.shape[2]
    cap = max(2, 3 * rows // (2 * n_exp))
    n_chip = n_exp // 2
    depth = dense_in.shape[0]
    half_y = n_cut // 2
    dims = (n_exp, n_cut, cap, rows, width, share, hidden)
    vmem = pl.BlockSpec(memory_space=pltpu.VMEM)
    hbm = pl.BlockSpec(memory_space=pltpu.HBM)
    dma = pltpu.SemaphoreType.DMA
    return pl.pallas_call(
        functools.partial(layer_kernel, dims),
        out_shape=jax.ShapeDtypeStruct((rows, share), BF16),
        in_specs=[hbm] * 8,
        out_specs=vmem,
        scratch_shapes=[
            pltpu.VMEM((1, rows), jnp.int32),
            pltpu.VMEM((1, rows), F32),
            pltpu.VMEM((1, width), F32),
            pltpu.VMEM((rows, 128), F32),
            pltpu.VMEM((rows, width), BF16),
            pltpu.VMEM((rows, width), BF16),
            pltpu.VMEM((n_exp * cap, rows), BF16),
            pltpu.VMEM((rows, n_exp * cap), BF16),
            pltpu.VMEM((rows, 128), F32),
            pltpu.VMEM((n_exp, cap, share), BF16),
            pltpu.VMEM((n_cut, 2, cap, share), BF16),
            pltpu.VMEM((n_cut, n_exp, cap, share), BF16),
            pltpu.VMEM((width, hidden), BF16),
            pltpu.VMEM((hidden, width), BF16),
            pltpu.VMEM((n_chip, 2, depth, hidden), BF16),
            pltpu.VMEM((n_chip, 2, hidden, depth), BF16),
            pltpu.VMEM((-(-n_exp // CHUNKS) * cap, hidden), BF16),
            pltpu.VMEM((n_cut, n_exp, cap, share), BF16),
            pltpu.VMEM((n_cut, 2, cap, share), BF16),
            pltpu.VMEM((2, half_y, n_exp, cap, share), BF16),
            pltpu.VMEM((n_cut, 6, cap, share), BF16),
            pltpu.VMEM((n_exp, cap, share), BF16),
            pltpu.VMEM((n_exp, cap, share), BF16),
            pltpu.VMEM((rows, hidden), BF16),
            pltpu.VMEM((n_cut, rows, share), BF16),
            pltpu.VMEM((2, half_y, rows, share), BF16),
            pltpu.VMEM((rows, share), F32),
            pltpu.VMEM((rows, 6 * cap), BF16),
            dma((7 + BLOCKS,)),
            dma((2,)),
            dma((2,)),
            dma,
            dma((CHUNKS,)),
            dma,
            dma((2, half_y, CHUNKS)),
            dma((2,)),
            dma((2, 2, 2, n_chip // 2)),
            dma((2,)),
            dma((2,)),
            dma,
            dma((2, half_y, CHUNKS)),
            dma,
            dma,
            dma,
            dma((2, half_y, CHUNKS)),
            dma,
            dma((half_y,)),
        ],
        compiler_params=pltpu.CompilerParams(
            collective_id=0, has_side_effects=True, vmem_limit_bytes=52 * 1024 * 1024
        ),
        name="moe_layer",
    )(
        *(
            pltpu.with_memory_space_constraint(operand, pltpu.HBM)
            for operand in (
                tokens,
                route.reshape(1, rows),
                gate_prob.reshape(1, rows),
                norm_gain.reshape(1, width),
                dense_in,
                dense_out,
                expert_in.reshape(width, hidden),
                expert_out.reshape(hidden, width),
            )
        )
    )


def solution(mesh):
    return jax.shard_map(
        local,
        mesh=mesh,
        in_specs=(
            P(("groups", "expert"), None),
            P(("groups", "expert"), None),
            P(("groups", "expert")),
            P(),
            P("expert", "cuts"),
            P("cuts", "expert"),
            P("expert", None, "cuts"),
            P("expert", "cuts", None),
        ),
        out_specs=P(("groups", "expert"), "cuts"),
        check_vma=False,
    )
```

```python
import functools

import jax
import jax.numpy as jnp
from jax import lax
from jax.experimental import pallas as pl
from jax.experimental.pallas import tpu as pltpu
from jax.sharding import PartitionSpec as P

MESH = pl.DeviceIdType.MESH
F32 = jnp.float32
BF16 = jnp.bfloat16
CHUNKS = 4
BLOCKS = 4


ORDER = (
    ("ring_own", 0), ("gather", 0, 0), ("gather", 0, 1), ("gather", 1, 0), ("gather", 0, 2),
    ("gather", 1, 1), ("gather", 0, 3), ("ring", 0, 0, 1), ("gather", 2, 0), ("ring", 0, 1, 1),
    ("gather", 1, 2), ("ring", 0, 0, 2), ("gather", 2, 1), ("gather", 1, 3), ("ring", 0, 1, 2),
    ("ring_own", 1), ("gather", 3, 0), ("gather", 2, 2), ("ring", 0, 0, 3), ("gather", 3, 1),
    ("ring", 0, 1, 3), ("gather", 2, 3), ("gather", 4, 0), ("expert", 0), ("ring", 1, 0, 1),
    ("gather", 3, 2), ("gather", 4, 1), ("expert", 1), ("gather", 3, 3), ("ered", 4, 1),
    ("gather", 4, 2), ("ring", 1, 1, 1), ("expert", 2), ("ring", 0, 0, 4), ("ring", 0, 1, 4),
    ("ered", 4, 2), ("gather", 4, 3), ("expert", 3), ("ered", 3, 1), ("ring", 1, 0, 2),
    ("ered", 4, 3), ("dfirst", 0), ("ered", 3, 2), ("ring", 1, 1, 2), ("nrsend", 0),
    ("dfirst", 1), ("ered", 2, 1), ("ered", 3, 3), ("ring", 1, 0, 3), ("ered", 2, 2),
    ("ring", 1, 1, 3), ("nrsend", 1), ("nrsend", 2), ("nrsend", 3), ("ered", 1, 1),
    ("ered", 2, 3), ("ring", 1, 0, 4), ("ered", 1, 2), ("ring", 1, 1, 4), ("ered", 1, 3),
    ("dsecond", 0), ("dred", 4, 0), ("dred", 4, 1), ("dred", 4, 2), ("dred", 4, 3), ("home", 1),
    ("home", 2), ("dsecond", 1), ("home", 3), ("dred", 3, 0), ("dsecond", 2), ("dred", 3, 1),
    ("dred", 3, 2), ("dred", 3, 3), ("dsecond", 3), ("dred", 2, 0), ("dred", 2, 1),
    ("dred", 2, 2), ("dred", 2, 3), ("dred", 1, 0), ("dred", 1, 1), ("base",), ("dred", 1, 2),
    ("dred", 1, 3), ("last", 0), ("last", 1), ("last", 2), ("last", 3),
)


def layer_kernel(
    dims,
    tokens_hbm,
    route_hbm,
    gate_hbm,
    gain_hbm,
    dense_in_hbm,
    dense_out_hbm,
    expert_in_hbm,
    expert_out_hbm,
    out_ref,
    route_ref,
    gate_ref,
    gain_ref,
    scale,
    tok,
    norm,
    pick,
    pick_home,
    gate_wide,
    outgoing,
    outgoing_near,
    arrived,
    w_in,
    w_out,
    d_in,
    d_out,
    inner,
    part,
    part_near,
    part_in,
    near,
    result,
    returned,
    dense_act,
    dense_part,
    dense_part_in,
    base,
    near_home,
    load_sem,
    near_send,
    near_recv,
    disp_send,
    disp_recv,
    gath_send,
    gath_recv,
    ring_send,
    ring_recv,
    sib_send,
    sib_recv,
    red_send,
    red_recv,
    ret_send,
    ret_recv,
    dred_send,
    dred_recv,
    next_sem,
    next_recv,
):
    n_exp, n_cut, cap, rows, width, share, hidden = dims
    n_chip = n_exp // 2
    half_x, half_y = n_chip // 2, n_cut // 2
    offsets = [0] + [(p + 1) // 2 if p % 2 else -(p // 2) for p in range(1, n_chip)]
    far = n_exp - 2
    size = -(-far // CHUNKS)
    size += size % 2
    chunks = [(first, min(size, n_exp - first)) for first in range(2, n_exp, size)]
    dsize = rows // CHUNKS
    dense_chunks = [(first, dsize) for first in range(0, rows, dsize)]

    e = lax.axis_index("expert")
    c = lax.axis_index("cuts")
    x = e // 2
    core = e - 2 * x
    other = 1 - core
    sibling = {"expert": 2 * x + other}

    def chip(offset):
        return lax.rem(x + offset + n_chip, n_chip)

    def cut(offset):
        return lax.rem(c + offset + n_cut, n_cut)

    def ring_device(way):
        return {"expert": 2 * chip(1 if way == 0 else -1) + core}

    def cut_device(way):
        return {"cuts": cut(1 if way == 0 else -1)}

    def remote(src, dst, send_sem, recv_sem, device):
        return pltpu.make_async_remote_copy(
            src_ref=src,
            dst_ref=dst,
            send_sem=send_sem,
            recv_sem=recv_sem,
            device_id=device,
            device_id_type=MESH,
        )

    def send(src, dst, send_sem, recv_sem, device):
        remote(src, dst, send_sem, recv_sem, device).start()

    def arrive(dst, recv_sem, send_sem):
        remote(dst, dst, send_sem, recv_sem, sibling).wait_recv()

    def sent(src, send_sem, recv_sem):
        remote(src, src, send_sem, recv_sem, sibling).wait_send()

    def halves(chunk):
        first, count = chunk
        return (
            pl.ds(first, count // 2),
            pl.ds(first + count // 2, count // 2),
        )

    block = rows // BLOCKS
    blocks = [pl.ds(n * block, block) for n in range(BLOCKS)]
    copies = [
        (expert_in_hbm, w_in),
        (expert_out_hbm, w_out),
        (dense_in_hbm, d_in.at[x, core]),
        (dense_out_hbm, d_out.at[x, core]),
        (route_hbm, route_ref),
        (gain_hbm, gain_ref),
        (gate_hbm, gate_ref),
    ]
    copies += [(tokens_hbm.at[here], tok.at[here]) for here in blocks]
    loads = [
        pltpu.make_async_copy(src, dst, load_sem.at[number])
        for number, (src, dst) in enumerate(copies)
    ]
    for copy in loads[4:]:
        copy.start()

    barrier = pltpu.get_barrier_semaphore()
    for step in range(1, n_exp):
        pl.semaphore_signal(
            barrier, inc=1, device_id={"expert": lax.rem(e + step, n_exp)}, device_id_type=MESH
        )
    for way in range(2):
        pl.semaphore_signal(barrier, inc=1, device_id=cut_device(way), device_id_type=MESH)

    loads[4].wait()
    route = route_ref[...]
    hot = lax.broadcasted_iota(jnp.int32, (n_exp, rows), 0) == route
    hot = jnp.where(hot, 1.0, 0.0).astype(F32)
    earlier = lax.broadcasted_iota(jnp.int32, (rows, rows), 0) < lax.broadcasted_iota(
        jnp.int32, (rows, rows), 1
    )
    earlier = jnp.where(earlier, 1.0, 0.0).astype(BF16)
    before = jnp.dot(hot.astype(BF16), earlier, preferred_element_type=F32)
    position = jnp.sum(before * hot, axis=0, keepdims=True)
    target = route * cap + position.astype(jnp.int32)
    slots = lax.broadcasted_iota(jnp.int32, (n_exp * cap, rows), 0)
    pick[...] = jnp.where(slots == target, 1.0, 0.0).astype(BF16)

    own_columns = pl.ds(pl.multiple_of(c * share, share), share)
    loads[5].wait()
    for n, here in enumerate(blocks):
        loads[7 + n].wait()
        wide = tok[here, :].astype(F32)
        factor = lax.rsqrt(jnp.mean(wide * wide, axis=-1, keepdims=True) + 1e-06)
        scale[here, :] = jnp.broadcast_to(factor, (block, 128))
        norm[here, own_columns] = (
            tok[here, own_columns].astype(F32) * factor * gain_ref[:, own_columns]
        ).astype(BF16)
    for number in (2, 3, 0, 1):
        loads[number].start()
    outgoing[...] = (
        jnp.dot(pick[...], norm[:, own_columns], preferred_element_type=F32)
        .astype(BF16)
        .reshape(n_exp, cap, share)
    )
    pl.semaphore_wait(barrier, n_exp + 1)

    def chunk_of(slot):
        return (slot - 2) // size

    for p in range(1, n_chip):
        for k in range(2):
            to = 2 * chip(-offsets[p]) + k
            send(
                outgoing.at[to],
                arrived.at[c, 2 * p + core],
                disp_send,
                disp_recv.at[chunk_of(2 * p)],
                {"expert": to},
            )

    @pl.loop(0, 8)
    def _(n):
        here = pl.ds(pl.multiple_of(n * (rows // 8), rows // 8), rows // 8)
        wide = tok[here, :].astype(F32)
        norm[here, :] = (wide * scale[here, 0:1] * gain_ref[...]).astype(BF16)

    near_rows = pick[pl.ds(pl.multiple_of(2 * x * cap, 2 * cap), 2 * cap), :]
    for k in range(n_cut):
        outgoing_near[k] = (
            jnp.dot(near_rows, norm[:, pl.ds(k * share, share)], preferred_element_type=F32)
            .astype(BF16)
            .reshape(2, cap, share)
        )
    send(
        outgoing_near.at[:, other], arrived.at[:, core], near_send.at[0], near_recv.at[0], sibling
    )
    for k in range(n_cut):
        arrived[k, core] = outgoing_near[k, core]

    weights = (d_in, d_out)

    def ring_piece(w, origin, p):
        half = weights[w].shape[2] // 2
        return weights[w].at[origin, core, pl.ds(p * half, half)]

    def ring_own(w):
        loads[2 + w].wait()
        for p in range(2):
            piece = ring_piece(w, x, p)
            for way in range(2):
                send(piece, piece, ring_send.at[w], ring_recv.at[way, w, p, 0], ring_device(way))
        own = weights[w].at[x, core]
        send(own, own, sib_send.at[w], sib_recv.at[w], sibling)

    def ring_event(w, p, hop):
        for way in range(2):
            if hop == half_x and p != way:
                continue
            piece = ring_piece(w, chip(-hop if way == 0 else hop), p)
            arrive(piece, ring_recv.at[way, w, p, hop - 1], ring_send.at[w])
            if hop < half_x - 1 or (hop == half_x - 1 and p == way):
                send(piece, piece, ring_send.at[w], ring_recv.at[way, w, p, hop], ring_device(way))
            send(piece, piece, sib_send.at[w], sib_recv.at[w], sibling)

    def gather_event(hop, r):
        first, count = chunks[r]
        whole = pl.ds(first, count)
        if hop == 0:
            arrive(arrived.at[c, whole], disp_recv.at[r], disp_send)
        for way in range(2):
            here = halves(chunks[r])[way] if hop == half_y else whole
            onward = halves(chunks[r])[way] if hop == half_y - 1 else here
            origin = cut(-hop if way == 0 else hop)
            if hop > 0:
                arrive(arrived.at[origin, here], gath_recv.at[way, hop - 1, r], gath_send)
            if hop < half_y:
                piece = arrived.at[origin, onward]
                send(piece, piece, gath_send, gath_recv.at[way, hop, r], cut_device(way))

    def expert_rows(first, count, keep):
        flat = jnp.concatenate(
            [
                arrived[k, pl.ds(first, count)].reshape(count * cap, share)
                for k in range(n_cut)
            ],
            axis=1,
        )
        for n in range(2):
            columns = pl.ds(n * (hidden // 2), hidden // 2)
            inner[pl.ds(0, count * cap), columns] = jax.nn.gelu(
                jnp.dot(flat, w_in[:, columns], preferred_element_type=F32)
            ).astype(BF16)
        for k in range(0, n_cut, 2):
            both = jnp.dot(
                inner[pl.ds(0, count * cap), :],
                w_out[:, pl.ds(k * share, 2 * share)],
                preferred_element_type=F32,
            ).astype(BF16)
            for j in range(2):
                keep(k + j, both[:, j * share : (j + 1) * share].reshape(count, cap, share))

    def expert_near():
        def keep(k, values):
            part_near[k] = values

        arrive(arrived.at[:, other], near_recv.at[0], near_send.at[0])
        expert_rows(0, 2, keep)
        send(
            part_near.at[:, other], near.at[:, core], near_send.at[1], near_recv.at[1], sibling
        )
        for k in range(n_cut):
            near[k, core] = part_near[k, core]

    pairs = [(half_y, half_y - 1)]
    pairs += [(-step, step - 1) for step in range(half_y - 1, 0, -1)]

    def next_send(i):
        for offset in pairs[i]:
            k = cut(offset)
            for slot in range(2, 6):
                send(
                    part.at[k, slot],
                    near.at[k, slot // 2 * 2 + core],
                    next_sem,
                    next_recv.at[i],
                    {"expert": 2 * chip(offsets[slot // 2]) + slot % 2},
                )

    def expert_chunk(r):
        first, count = chunks[r]

        def keep(k, values):
            part[k, pl.ds(first, count)] = values

        expert_rows(first, count, keep)

    def reduce_event(own, landed, send_sem, recv_sem, chunk, step, r):
        whole = pl.ds(*chunk)
        for way in range(2):
            half, rest = halves(chunk)[way], halves(chunk)[1 - way]
            home = cut(step if way == 0 else -step)
            to = step - 1
            if step == half_y:
                send(
                    own.at[home, half],
                    landed.at[way, to, half],
                    send_sem,
                    recv_sem.at[way, to, r],
                    cut_device(way),
                )
                continue
            here = half if step == half_y - 1 else whole
            arrive(landed.at[way, step, here], recv_sem.at[way, step, r], send_sem)
            landed[way, step, here] = (
                landed[way, step, here].astype(F32) + own[home, here].astype(F32)
            ).astype(BF16)
            if step == half_y - 1:
                landed[way, step, rest] = own[home, rest]
            send(
                landed.at[way, step, whole],
                landed.at[way, to, whole],
                send_sem,
                recv_sem.at[way, to, r],
                cut_device(way),
            )

    def reduce_last(own, landed, send_sem, recv_sem, chunk, r):
        whole = pl.ds(*chunk)
        total = own[c, whole].astype(F32)
        for way in range(2):
            arrive(landed.at[way, 0, whole], recv_sem.at[way, 0, r], send_sem)
            total = total + landed[way, 0, whole].astype(F32)
        return total

    def expert_reduce(step, r):
        reduce_event(part, part_in, red_send, red_recv, chunks[r], step, r)

    def go_home(r):
        first, count = chunks[r]
        result[pl.ds(first, count)] = reduce_last(
            part, part_in, red_send, red_recv, chunks[r], r
        ).astype(BF16)
        for slot in range(first, first + count):
            to = 2 * chip(offsets[slot // 2]) + slot % 2
            send(result.at[slot], returned.at[e], ret_send, ret_recv, {"expert": to})

    def dense_first(n):
        if n == 0:
            arrive(d_in.at[:, other], sib_recv.at[0], sib_send.at[0])
        columns = pl.ds(n * (hidden // 2), hidden // 2)
        dense_act[:, columns] = jax.nn.gelu(
            jnp.dot(
                norm[...],
                d_in[:, :, :, columns].reshape(width, hidden // 2),
                preferred_element_type=F32,
            )
        ).astype(BF16)

    def dense_second(i):
        if i == 0:
            arrive(d_out.at[:, other], sib_recv.at[1], sib_send.at[1])
            arrive(near.at[:, other], near_recv.at[1], near_send.at[1])
        arrive(near.at[pl.ds(0, 2), pl.ds(2, 4)], next_recv.at[i], next_sem)
        ks = [cut(offset) for offset in pairs[i]]
        both = jnp.dot(
            dense_act[...],
            jnp.concatenate([d_out[k, j] for k in ks for j in range(2)], axis=1),
            preferred_element_type=F32,
        )
        rows_near = jnp.concatenate([near[k].reshape(6 * cap, share) for k in ks], axis=1)
        both = both + gate_wide[:, 0:1] * jnp.dot(
            near_home[...], rows_near, preferred_element_type=F32
        )
        both = both.astype(BF16)
        dense_part[ks[0]] = both[:, :share]
        dense_part[ks[1]] = both[:, share:]

    def dense_reduce(step, r):
        reduce_event(
            dense_part, dense_part_in, dred_send, dred_recv, dense_chunks[r], step, r
        )

    def home_tables():
        gate_wide[...] = jnp.transpose(jnp.broadcast_to(gate_ref[...], (128, rows)))
        wide = jnp.transpose(jnp.broadcast_to(target.astype(F32), (128, rows)))[:, 0:1]
        slot_of = lax.broadcasted_iota(jnp.int32, (rows, n_exp * cap), 1).astype(F32)
        pick_home[...] = jnp.where(slot_of == wide, 1.0, 0.0).astype(BF16)
        lane = lax.broadcasted_iota(jnp.int32, (rows, 6 * cap), 1)
        first = jnp.where(
            lane < 2 * cap,
            2 * cap * x,
            jnp.where(
                lane < 4 * cap, 2 * cap * (chip(-1) - 1), 2 * cap * (chip(1) - 2)
            ),
        )
        near_home[...] = jnp.where((lane + first).astype(F32) == wide, 1.0, 0.0).astype(BF16)

    def dense_base():
        arrive(returned.at[pl.ds(0, far - 4)], ret_recv, ret_send)
        expert_res = jnp.dot(
            pick_home[...],
            returned[...].reshape(n_exp * cap, share),
            preferred_element_type=F32,
        )
        base[...] = tok[:, own_columns].astype(F32) + gate_wide[:, 0:1] * expert_res

    def dense_last(r):
        here = pl.ds(*dense_chunks[r])
        total = reduce_last(dense_part, dense_part_in, dred_send, dred_recv, dense_chunks[r], r)
        out_ref[here, :] = (base[here, :] + total).astype(BF16)

    for offset in (-1, 0, 1):
        returned[pl.ds(2 * chip(offset), 2)] = jnp.zeros((2, cap, share), BF16)

    ring_own(0)
    loads[6].wait()
    home_tables()
    loads[0].wait()
    loads[1].wait()
    expert_near()
    steps = {
        "gather": gather_event,
        "ring_own": ring_own,
        "ring": ring_event,
        "expert": expert_chunk,
        "nrsend": next_send,
        "ered": expert_reduce,
        "home": go_home,
        "dfirst": dense_first,
        "dsecond": dense_second,
        "dred": dense_reduce,
        "base": dense_base,
        "last": dense_last,
    }
    for name, *where in ORDER:
        if (name, *where) != ("ring_own", 0):
            steps[name](*where)

    sent(outgoing.at[pl.ds(0, far)], disp_send, disp_recv.at[0])
    sent(outgoing_near.at[:, 0], near_send.at[0], near_recv.at[0])
    sent(part_near.at[:, 0], near_send.at[1], near_recv.at[1])
    sent(arrived.at[pl.ds(0, n_cut - 1), pl.ds(2, far)], gath_send, gath_recv.at[0, 0, 0])
    for w in range(2):
        sent(weights[w].at[pl.ds(0, n_chip - 1), 0], ring_send.at[w], ring_recv.at[0, w, 0, 0])
        sent(weights[w].at[:, 0], sib_send.at[w], sib_recv.at[w])
    sent(part.at[:, pl.ds(2, 4)], next_sem, next_recv.at[0])
    sent(part.at[pl.ds(0, n_cut - 1), pl.ds(6, far - 4)], red_send, red_recv.at[0, 0, 0])
    sent(result.at[pl.ds(6, far - 4)], ret_send, ret_recv)
    sent(dense_part.at[pl.ds(0, n_cut - 1)], dred_send, dred_recv.at[0, 0, 0])


def local(tokens, route, gate_prob, norm_gain, dense_in, dense_out, expert_in, expert_out):
    n_exp = lax.axis_size("expert")
    n_cut = lax.axis_size("cuts")
    rows, width = tokens.shape
    share = width // n_cut
    hidden = expert_in.shape[2]
    cap = max(2, 3 * rows // (2 * n_exp))
    n_chip = n_exp // 2
    depth = dense_in.shape[0]
    half_y = n_cut // 2
    dims = (n_exp, n_cut, cap, rows, width, share, hidden)
    vmem = pl.BlockSpec(memory_space=pltpu.VMEM)
    hbm = pl.BlockSpec(memory_space=pltpu.HBM)
    dma = pltpu.SemaphoreType.DMA
    return pl.pallas_call(
        functools.partial(layer_kernel, dims),
        out_shape=jax.ShapeDtypeStruct((rows, share), BF16),
        in_specs=[hbm] * 8,
        out_specs=vmem,
        scratch_shapes=[
            pltpu.VMEM((1, rows), jnp.int32),
            pltpu.VMEM((1, rows), F32),
            pltpu.VMEM((1, width), F32),
            pltpu.VMEM((rows, 128), F32),
            pltpu.VMEM((rows, width), BF16),
            pltpu.VMEM((rows, width), BF16),
            pltpu.VMEM((n_exp * cap, rows), BF16),
            pltpu.VMEM((rows, n_exp * cap), BF16),
            pltpu.VMEM((rows, 128), F32),
            pltpu.VMEM((n_exp, cap, share), BF16),
            pltpu.VMEM((n_cut, 2, cap, share), BF16),
            pltpu.VMEM((n_cut, n_exp, cap, share), BF16),
            pltpu.VMEM((width, hidden), BF16),
            pltpu.VMEM((hidden, width), BF16),
            pltpu.VMEM((n_chip, 2, depth, hidden), BF16),
            pltpu.VMEM((n_chip, 2, hidden, depth), BF16),
            pltpu.VMEM((-(-n_exp // CHUNKS) * cap, hidden), BF16),
            pltpu.VMEM((n_cut, n_exp, cap, share), BF16),
            pltpu.VMEM((n_cut, 2, cap, share), BF16),
            pltpu.VMEM((2, half_y, n_exp, cap, share), BF16),
            pltpu.VMEM((n_cut, 6, cap, share), BF16),
            pltpu.VMEM((n_exp, cap, share), BF16),
            pltpu.VMEM((n_exp, cap, share), BF16),
            pltpu.VMEM((rows, hidden), BF16),
            pltpu.VMEM((n_cut, rows, share), BF16),
            pltpu.VMEM((2, half_y, rows, share), BF16),
            pltpu.VMEM((rows, share), F32),
            pltpu.VMEM((rows, 6 * cap), BF16),
            dma((7 + BLOCKS,)),
            dma((2,)),
            dma((2,)),
            dma,
            dma((CHUNKS,)),
            dma,
            dma((2, half_y, CHUNKS)),
            dma((2,)),
            dma((2, 2, 2, n_chip // 2)),
            dma((2,)),
            dma((2,)),
            dma,
            dma((2, half_y, CHUNKS)),
            dma,
            dma,
            dma,
            dma((2, half_y, CHUNKS)),
            dma,
            dma((half_y,)),
        ],
        compiler_params=pltpu.CompilerParams(
            collective_id=0, has_side_effects=True, vmem_limit_bytes=52 * 1024 * 1024
        ),
        name="moe_layer",
    )(
        *(
            pltpu.with_memory_space_constraint(operand, pltpu.HBM)
            for operand in (
                tokens,
                route.reshape(1, rows),
                gate_prob.reshape(1, rows),
                norm_gain.reshape(1, width),
                dense_in,
                dense_out,
                expert_in.reshape(width, hidden),
                expert_out.reshape(hidden, width),
            )
        )
    )


def solution(mesh):
    return jax.shard_map(
        local,
        mesh=mesh,
        in_specs=(
            P(("groups", "expert"), None),
            P(("groups", "expert"), None),
            P(("groups", "expert")),
            P(),
            P("expert", "cuts"),
            P("cuts", "expert"),
            P("expert", None, "cuts"),
            P("expert", "cuts", None),
        ),
        out_specs=P(("groups", "expert"), "cuts"),
        check_vma=False,
    )
```
